256 devices in a mesh: grp: 8 (over y, x_lo), tp: 32 (over z, x_hi, core).
Axes of the slice: x: 4 (x_hi: 2, x_lo: 2; x = x_hi * 2 + x_lo), y: 4, z: 8, core: 2. Of those that a mesh axis runs over, the one named last changes fastest.
Arguments:
- teacher_in: bfloat16 [384, 8192], P('tp', 'grp'), may hold values from -6 to 6
- teacher_gate: bfloat16 [8192, 28672], P('grp', 'tp'), may hold values from -0.0625 to 0.0625
- teacher_up: bfloat16 [8192, 28672], P('grp', 'tp'), may hold values from -0.0625 to 0.0625
- teacher_down: bfloat16 [28672, 8192], P('tp', 'grp'), may hold values from -0.0625 to 0.0625
- student_in: bfloat16 [384, 4096], P('tp', 'grp'), may hold values from -6 to 6
- student_gate: bfloat16 [4096, 14336], P('grp', 'tp'), may hold values from -0.09375 to 0.09375
- student_up: bfloat16 [4096, 14336], P('grp', 'tp'), may hold values from -0.09375 to 0.09375
- student_down: bfloat16 [14336, 4096], P('tp', 'grp'), may hold values from -0.046875 to 0.046875
- projector: bfloat16 [4096, 8, 1024], P('grp', None, 'tp'), may hold values from -0.09375 to 0.09375
Outputs:
- grad_input: float32 [384, 4096], P('tp', 'grp')
- grad_gate: float32 [4096, 14336], P('grp', 'tp')
- grad_up: float32 [4096, 14336], P('grp', 'tp')
- grad_down: float32 [14336, 4096], P('tp', 'grp')
- grad_projector: float32 [4096, 8, 1024], P('grp', None, 'tp')
The draws below stay inside these ranges and needn't reach their ends.
All inputs are finite; a program needn't handle non-finite values.
Results may differ from the reference program's by a relative error of at most 0.017.
Values may be sent and summed in bfloat16 or wider, within the bound.
A program may use at most 64 MiB of HBM per device.

```python
import jax
import jax.numpy as jnp

DT = 8192
FT = 28672
DS = 4096
FS = 14336
TOKENS = 384
N_GRP = 8


def strengthened(result, own_key, source, target, parts, factor):
    owner, partner = [(jnp.arange(result.shape[axis_at]) // (result.shape[axis_at] // parts)).reshape([-1 if axis == axis_at else 1 for axis in range(result.ndim)]) for axis_at in (source, target)]
    chosen = jax.random.permutation(own_key, parts)[partner]
    strong = (owner == chosen) | (owner == (partner + parts // 2) % parts)
    return jnp.where(strong, factor * result, result)


def shard_levels(stream_key, dims, pieces, least, high):
    level = 1.0
    for position, parts in pieces:
        heights = jax.random.uniform(jax.random.fold_in(jax.random.fold_in(stream_key, 6), position), (parts,), jnp.float32, least / len(pieces), high / len(pieces))
        level = level * jnp.repeat(jnp.exp(heights), dims[position] // parts).reshape((-1,) + (1,) * (len(dims) - 1 - position))
    return level


def gaussian(stream_key, dims, scale, reach, split=(), dtype=jnp.bfloat16):
    result = scale * jax.random.normal(stream_key, dims, jnp.float32)
    if split:
        result = result * shard_levels(stream_key, dims, split, -0.22, 0.18)
    return jnp.clip(result, -reach, reach).astype(dtype)


def bell_draw_with(own_key, extent, deviation, reach, cuts, heavy, held_as=jnp.bfloat16):
    values = deviation * jax.random.normal(own_key, extent, jnp.float32)
    if cuts:
        values = values * shard_levels(own_key, extent, cuts, -0.22, 0.18)
    return jnp.clip(strengthened(values, jax.random.fold_in(own_key, 3), *heavy), -reach, reach).astype(held_as)


def setup_inputs(seed: int = 0) -> dict:
    arg_keys = jax.random.split(jax.random.key(seed), 10)
    teacher_in = gaussian(arg_keys[0], (TOKENS, DT), 1.0, 6.0, ((0, 32), (1, 8)))
    teacher_gate = gaussian(arg_keys[1], (DT, FT), DT ** -0.5, 0.0625, ((0, 8), (1, 32)))
    teacher_up = gaussian(arg_keys[2], (DT, FT), DT ** -0.5, 0.0625, ((0, 8), (1, 32)))
    teacher_down = bell_draw_with(arg_keys[3], (FT, DT), FT ** -0.5, 0.0625, ((0, 32), (1, 8)), (0, 1, 32, 2.75))
    student_in = gaussian(arg_keys[4], (TOKENS, DS), 1.0, 6.0, ((0, 32), (1, 8)))
    student_gate = gaussian(arg_keys[5], (DS, FS), DS ** -0.5, 0.09375, ((0, 8), (1, 32)))
    student_up = gaussian(arg_keys[6], (DS, FS), DS ** -0.5, 0.09375, ((0, 8), (1, 32)))
    student_down = gaussian(arg_keys[7], (FS, DS), FS ** -0.5, 0.046875, ((0, 32), (1, 8)))
    projector = gaussian(arg_keys[8], (DS, N_GRP, DT // N_GRP), DS ** -0.5, 0.09375, ((0, 8), (2, 32)))
    return dict(teacher_in=teacher_in, teacher_gate=teacher_gate, teacher_up=teacher_up, teacher_down=teacher_down, student_in=student_in, student_gate=student_gate, student_up=student_up, student_down=student_down, projector=projector)


def reference(teacher_in, teacher_gate, teacher_up, teacher_down, student_in, student_gate, student_up, student_down, projector):
    bf = jnp.bfloat16
    fl = jnp.float32
    teacher_pre = jnp.dot(teacher_in, teacher_gate, preferred_element_type=fl)
    teacher_lin = jnp.dot(teacher_in, teacher_up, preferred_element_type=fl)
    teacher_hidden = (jax.nn.silu(teacher_pre) * teacher_lin).astype(bf)
    teacher_feature = jnp.dot(teacher_hidden, teacher_down, preferred_element_type=fl).astype(bf)
    gate_values = jnp.dot(student_in, student_gate, preferred_element_type=fl)
    up_values = jnp.dot(student_in, student_up, preferred_element_type=fl)
    student_hidden = (jax.nn.silu(gate_values) * up_values).astype(bf)
    student_feature = jnp.dot(student_hidden, student_down, preferred_element_type=fl).astype(bf)
    proj_matrix = projector.reshape(projector.shape[0], -1)
    projected = jnp.dot(student_feature, proj_matrix, preferred_element_type=fl)
    residual_grad = (projected - teacher_feature.astype(fl)).astype(bf)
    grad_projector = jnp.dot(student_feature.T, residual_grad, preferred_element_type=fl).reshape(projector.shape)
    feature_grad = jnp.dot(residual_grad, proj_matrix.T, preferred_element_type=fl).astype(bf)
    grad_down = jnp.dot(student_hidden.T, feature_grad, preferred_element_type=fl)
    hidden_grad = jnp.dot(feature_grad, student_down.T, preferred_element_type=fl)
    sigmoid_gate = jax.nn.sigmoid(gate_values)
    gate_grad = (hidden_grad * up_values * sigmoid_gate * (1.0 + gate_values * (1.0 - sigmoid_gate))).astype(bf)
    up_grad = (hidden_grad * gate_values * sigmoid_gate).astype(bf)
    grad_gate = jnp.dot(student_in.T, gate_grad, preferred_element_type=fl)
    grad_up = jnp.dot(student_in.T, up_grad, preferred_element_type=fl)
    grad_input = jnp.dot(gate_grad, student_gate.T, preferred_element_type=fl) + jnp.dot(up_grad, student_up.T, preferred_element_type=fl)
    return grad_input, grad_gate, grad_up, grad_down, grad_projector
```

```python
import functools

import jax
import jax.numpy as jnp
from jax import lax
from jax.experimental import pallas as pl
from jax.experimental.pallas import tpu as pltpu
from jax.sharding import Mesh
from jax.sharding import PartitionSpec as P

AXES = ("y", "xl", "z", "xh", "c")
TP = ("z", "xh", "c")
GRP = ("y", "xl")
BF = jnp.bfloat16
FL = jnp.float32


def dot(a, b, ca, cb):
    return lax.dot_general(a, b, (((ca,), (cb,)), ((), ())), preferred_element_type=FL)


def kernel(
    sizes,
    t_in, t_gate, t_up, t_down, s_in, s_gate, s_up, s_down, proj_t,
    o_x, o_h, o_f, o_rt, o_fg, o_gg, o_ug, o_gi,
    w_tg, w_tu, w_td, w_tdt, w_sp, w_sd, w_pt,
    xs, xtmp, x, s2s, s2r, pv, h,
    f_keep, f_cs, f_cr, f_rs, f_rr, f,
    p_s, p_r, rt,
    g_keep, g_cs, g_cr, g_rs, g_rr, fg,
    h_s, h_r, gu, gg, ug,
    gi_f, gi_cs, gi_cr, gi_rs, gi_rr, gi,
    ts, ttmp, tx, t2s, t2r, t2a, th,
    tf_keep, tf_cs, tf_cr, tf_rs, tf_rr, tf,
    w_sem, i_sem, o_sem, grp_ss, grp_rs, tp_ss, tp_rs, fw_ss, fw_rs, c_ss, c_rs,
):
    Y, XL, Z, XH = sizes
    G = Y * XL
    N = Z * XH
    y = lax.axis_index("y")
    xl = lax.axis_index("xl")
    z = lax.axis_index("z")
    xh = lax.axis_index("xh")
    c = lax.axis_index("c")
    o = 1 - c
    g = y * XL + xl
    RZ = x.shape[0] // Z
    RB = RZ // (2 * XH)

    def grp_to(k):
        return {"y": lax.rem(y + k // XL, Y), "xl": lax.rem(xl + lax.rem(k, XL), XL)}

    def grp_from(k):
        return lax.rem(y + Y - k // XL, Y) * XL + lax.rem(xl + XL - lax.rem(k, XL), XL)

    def tp_to(k):
        return {"z": lax.rem(z + k // XH, Z), "xh": lax.rem(xh + lax.rem(k, XH), XH)}

    def tp_from(k):
        return lax.rem(z + Z - k // XH, Z), lax.rem(xh + XH - lax.rem(k, XH), XH)

    other = {"c": o}

    def rdma(src, dst, ss, rs, dev):
        return pltpu.make_async_remote_copy(
            src_ref=src, dst_ref=dst, send_sem=ss, recv_sem=rs,
            device_id=dev, device_id_type=pl.DeviceIdType.MESH,
        )

    def loop(lo, hi, body):
        def step(i, carry):
            body(i)
            return carry

        lax.fori_loop(lo, hi, step, 0)

    late = []

    def grp_rs_copy(ph, k, send, recv):
        to = grp_to(k)
        return rdma(
            send.at[to["y"] * XL + to["xl"]], recv.at[k - 1],
            grp_ss.at[ph, k], grp_rs.at[ph, k], to,
        )

    def grp_rs_start(ph, send, recv):
        loop(1, G, lambda k: grp_rs_copy(ph, k, send, recv).start())
        late.append(lambda: loop(1, G, lambda k: grp_rs_copy(ph, k, send, recv).wait_send()))

    def grp_ag_copy(ph, k, buf, at):
        return rdma(buf.at[at(g)], buf.at[at(g)], grp_ss.at[ph, k], grp_rs.at[ph, k], grp_to(k))

    def grp_ag_start(ph, buf, at):
        loop(1, G, lambda k: grp_ag_copy(ph, k, buf, at).start())
        late.append(lambda: loop(1, G, lambda k: grp_ag_copy(ph, k, buf, at).wait_send()))

    def grp_ag_wait(ph, buf, at):
        def one(k):
            src = grp_from(k)
            rdma(
                buf.at[at(src)], buf.at[at(src)], grp_ss.at[ph, k], grp_rs.at[ph, k], grp_to(k)
            ).wait_recv()

        loop(1, G, one)

    def tp_ag_start(ph, buf, at):
        mine = buf.at[at(z, xh, c)]
        loop(1, N, lambda k: rdma(mine, mine, tp_ss.at[ph, k], tp_rs.at[ph, k], tp_to(k)).start())
        rdma(mine, mine, fw_ss.at[ph, 0], fw_rs.at[ph, 0], other).start()
        late.append(
            lambda: loop(
                1, N, lambda k: rdma(mine, mine, tp_ss.at[ph, k], tp_rs.at[ph, k], tp_to(k)).wait_send()
            )
        )
        late.append(
            lambda: loop(
                0, N, lambda k: rdma(mine, mine, fw_ss.at[ph, k], fw_rs.at[ph, k], other).wait_send()
            )
        )

    def tp_ag_forward(ph, buf, at):
        def one(k):
            zz, xx = tp_from(k)
            block = buf.at[at(zz, xx, c)]
            rdma(block, block, tp_ss.at[ph, k], tp_rs.at[ph, k], tp_to(k)).wait_recv()
            rdma(block, block, fw_ss.at[ph, k], fw_rs.at[ph, k], other).start()

        loop(1, N, one)

    def tp_ag_wait(ph, buf, at):
        def one(k):
            zz, xx = tp_from(k)
            block = buf.at[at(zz, xx, o)]
            rdma(block, block, fw_ss.at[ph, k], fw_rs.at[ph, k], other).wait_recv()

        loop(0, N, one)

    def c_copy(ph, src, dst):
        return rdma(src, dst, c_ss.at[ph], c_rs.at[ph], other)

    def c_start(ph, src, dst):
        c_copy(ph, src, dst).start()
        late.append(lambda: c_copy(ph, src, dst).wait_send())

    def tp_rs_copy(ph, k, send, recv):
        to = tp_to(k)
        return rdma(
            send.at[to["z"] * XH + to["xh"]], recv.at[k - 1], tp_ss.at[ph, k], tp_rs.at[ph, k], to
        )

    def tp_rs_start(ph, send, recv):
        loop(1, N, lambda k: tp_rs_copy(ph, k, send, recv).start())
        late.append(lambda: loop(1, N, lambda k: tp_rs_copy(ph, k, send, recv).wait_send()))

    def summed(n, copy, recv, first):
        def step(k, acc):
            copy(k).wait_recv()
            return acc + recv[k - 1].astype(FL)

        return lax.fori_loop(1, n, step, first)

    def tp_rs_sum(ph, send, recv):
        return summed(N, lambda k: tp_rs_copy(ph, k, send, recv), recv, send[z * XH + xh].astype(FL))

    def grp_rs_sum(ph, send, recv):
        return summed(G, lambda k: grp_rs_copy(ph, k, send, recv), recv, send[g].astype(FL))

    FS_L = s_gate.shape[0]
    A = FS_L // 128 * 128
    B = FS_L - A
    loads = [
        pltpu.make_async_copy(src, dst, w_sem.at[i])
        for i, (src, dst) in enumerate(
            (
                (s_gate.at[:A], w_sp.at[:A]), (s_up.at[:A], w_sp.at[A : 2 * A]),
                (s_gate.at[A:], w_sp.at[2 * A : A + FS_L]), (s_up.at[A:], w_sp.at[A + FS_L :]),
                (t_gate, w_tg), (t_up, w_tu), (t_down, w_td), (s_down, w_sd), (proj_t, w_pt),
            )
        )
    ]
    in_s = pltpu.make_async_copy(s_in, xs.at[z, xh, c], i_sem.at[0])
    in_t = pltpu.make_async_copy(t_in, ts.at[z, xh, c], i_sem.at[1])
    in_s.start()
    in_t.start()
    for load in loads:
        load.start()

    def put(i, src, dst):
        copy = pltpu.make_async_copy(src, dst, o_sem.at[i])
        copy.start()
        late.append(copy.wait)

    barrier = pltpu.get_barrier_semaphore()

    def greet(dev):
        pl.semaphore_signal(barrier, inc=1, device_id=dev, device_id_type=pl.DeviceIdType.MESH)

    greet(other)
    loop(1, G, lambda k: greet(grp_to(k)))
    loop(1, N, lambda k: greet(tp_to(k)))
    pl.semaphore_wait(barrier, 1 + G - 1 + N - 1)

    def at_block(zz, xx, cc):
        return (zz, xx, cc)

    in_s.wait()
    tp_ag_start(0, xs, at_block)
    in_t.wait()
    tp_ag_start(1, ts, at_block)

    def compact(blocks, tmp, rows):
        def one(i):
            for q in range(2 * XH):
                tmp[q * RB : (q + 1) * RB, :] = blocks[i, q // 2, q % 2].astype(FL)
            rows[pl.ds(pl.multiple_of(i * RZ, 16), RZ), :] = tmp[...].astype(BF)

        loop(0, Z, one)

    tp_ag_forward(0, xs, at_block)
    tp_ag_wait(0, xs, at_block)
    compact(xs, xtmp, x)
    put(0, x, o_x)

    for i in range(4):
        loads[i].wait()
    rows_g = x.shape[0] // G
    half = x.shape[0]
    n0 = 0
    while n0 < 2 * FS_L:
        n1 = min(n0 + 256, 2 * FS_L)
        out = dot(x[...], w_sp[n0:n1, :], 1, 1).astype(BF)
        for i in range(G):
            s2s[i, :, n0:n1] = out[i * rows_g : (i + 1) * rows_g]
        n0 = n1
    grp_rs_start(0, s2s, s2r)

    tp_ag_forward(1, ts, at_block)
    loads[6].wait()
    FT_L, BT = w_td.shape
    for j in range(BT // 128):
        w_tdt[j * 128 : (j + 1) * 128, :] = w_td[:, j * 128 : (j + 1) * 128].T
    tp_ag_wait(1, ts, at_block)
    compact(ts, ttmp, tx)
    loads[4].wait()
    loads[5].wait()
    for j, w in enumerate((w_tg, w_tu)):
        n0 = 0
        while n0 < FT_L:
            n1 = min(n0 + 256, FT_L)
            out = dot(tx[...], w[:, n0:n1], 1, 0).astype(BF)
            for i in range(G):
                t2s[i, j, :, n0:n1] = out[i * rows_g : (i + 1) * rows_g]
            n0 = n1

    acc = grp_rs_sum(0, s2s, s2r)
    pv[:, : 2 * A] = acc[:, : 2 * A]
    pv[:, 2 * A : 2 * FS_L] = acc[:, 2 * A :]
    pv[:, 2 * FS_L :] = pltpu.roll(acc[:, 2 * A :], B, 1)

    def pair_values():
        return ((pv[:, :A], pv[:, A : 2 * A], slice(0, A)),
                (pv[:, 2 * A : 2 * FS_L], pv[:, 2 * FS_L :], slice(A, FS_L)))

    for gate, up, cols in pair_values():
        value = (gate * jax.nn.sigmoid(gate) * up).astype(BF)
        h[g, :, cols] = value[:, : cols.stop - cols.start]

    def at_g(i):
        return (i,)

    grp_ag_start(1, h, at_g)
    grp_rs_start(2, t2s, t2r)
    grp_ag_wait(1, h, at_g)
    put(1, h, o_h)

    def all_sum_start(ph, part, keep, cs, cr):
        w = part.shape[1] // 2
        for j in range(2):
            keep[j] = part[:, j * w : (j + 1) * w]
            cs[j] = part[:, j * w : (j + 1) * w].astype(BF)
        c_start(ph, cs.at[o], cr)

    def all_sum_scatter(ph, tph, keep, cs, cr, rs, rr):
        c_copy(ph, cs.at[o], cr).wait_recv()
        q = cr.shape[1] // XH
        for i in range(Z):
            rows = slice(i * RZ, (i + 1) * RZ)
            both = keep[c, rows, :] + cr[rows, :].astype(FL)
            for j in range(XH):
                rs[i * XH + j] = both[:, j * q : (j + 1) * q].astype(BF)
        tp_rs_start(tph, rs, rr)

    Q = f.shape[1] // (2 * XH)

    def at_tile(zz, xx, cc):
        return (
            pl.ds(pl.multiple_of(zz * RZ, 16), RZ),
            pl.ds(pl.multiple_of((cc * XH + xx) * Q, Q), Q),
        )

    loads[7].wait()
    hh = h[...].reshape(half, h.shape[2])
    all_sum_start(0, dot(hh, w_sd[...], 1, 0), f_keep, f_cs, f_cr)
    all_sum_scatter(0, 2, f_keep, f_cs, f_cr, f_rs, f_rr)
    f[at_tile(z, xh, c)] = tp_rs_sum(2, f_rs, f_rr).astype(BF)
    tp_ag_start(3, f, at_tile)

    t2a[...] = t2s[g].astype(FL)

    def t2_add(k):
        grp_rs_copy(2, k, t2s, t2r).wait_recv()
        t2a[...] += t2r[k - 1].astype(FL)

    loop(1, G, t2_add)
    t_pre = t2a[0]
    th[g] = (t_pre * jax.nn.sigmoid(t_pre) * t2a[1]).astype(BF)
    grp_ag_start(3, th, at_g)

    tp_ag_forward(3, f, at_tile)
    tp_ag_wait(3, f, at_tile)
    put(2, f, o_f)

    loads[8].wait()
    p_part = dot(w_pt[...], f[...], 1, 1).astype(BF)
    O = p_s.shape[1]
    for i in range(G):
        p_s[i] = p_part[i * O : (i + 1) * O]
    grp_rs_start(4, p_s, p_r)

    grp_ag_wait(3, th, at_g)
    thh = th[...].reshape(half, th.shape[2])
    per = BT // Z
    for i in range(Z):
        part = dot(w_tdt[i * per : (i + 1) * per, :], thh, 1, 1)
        for j in range(XH):
            for m in range(2):
                block = part[(j * 2 + m) * O : (j * 2 + m + 1) * O]
                tf_keep[m, i * XH + j] = block
                tf_cs[m, i * XH + j] = block.astype(BF)
    c_start(1, tf_cs.at[o], tf_cr)
    c_copy(1, tf_cs.at[o], tf_cr).wait_recv()
    for i in range(N):
        tf_rs[i] = (tf_keep[c, i] + tf_cr[i].astype(FL)).astype(BF)
    tp_rs_start(4, tf_rs, tf_rr)
    projected = grp_rs_sum(4, p_s, p_r)
    tf[...] = tp_rs_sum(4, tf_rs, tf_rr)

    rt[g] = (projected - tf[...].astype(BF).astype(FL)).astype(BF)
    grp_ag_start(5, rt, at_g)
    grp_ag_wait(5, rt, at_g)
    put(3, rt, o_rt)

    rtt = rt[...].reshape(G * O, half)
    all_sum_start(2, dot(rtt.T, w_pt[...], 1, 0), g_keep, g_cs, g_cr)
    all_sum_scatter(2, 5, g_keep, g_cs, g_cr, g_rs, g_rr)
    fg[at_tile(z, xh, c)] = tp_rs_sum(5, g_rs, g_rr).astype(BF)
    tp_ag_start(6, fg, at_tile)
    tp_ag_forward(6, fg, at_tile)
    tp_ag_wait(6, fg, at_tile)
    put(4, fg, o_fg)

    h_part = dot(fg[...], w_sd[...], 1, 1).astype(BF)
    for i in range(G):
        h_s[i] = h_part[i * rows_g : (i + 1) * rows_g]
    grp_rs_start(6, h_s, h_r)
    hidden_grad = grp_rs_sum(6, h_s, h_r)
    (gate, up, _), (gate_2, up_2, _) = pair_values()

    def pair_grads(grad, gate, up):
        s = jax.nn.sigmoid(gate)
        return grad * up * s * (1.0 + gate * (1.0 - s)), grad * gate * s

    gate_grad, up_grad = pair_grads(hidden_grad[:, :A], gate, up)
    gu[g, :, :A] = gate_grad.astype(BF)
    gu[g, :, A : 2 * A] = up_grad.astype(BF)
    rest = jnp.concatenate([hidden_grad[:, A:], hidden_grad[:, A:]], axis=1)
    gate_grad, up_grad = pair_grads(rest, gate_2, up_2)
    lane = lax.broadcasted_iota(jnp.int32, gate_grad.shape, 1)
    gu[g, :, 2 * A :] = jnp.where(lane < B, gate_grad, pltpu.roll(up_grad, B, 1)).astype(BF)

    grp_ag_start(7, gu, at_g)
    grp_ag_wait(7, gu, at_g)
    gur = gu[...].reshape(half, 2 * FS_L)

    gi_part = dot(gur, w_sp[...], 1, 0)
    gi_f[...] = gi_part.reshape(gi_f.shape)
    last = gur[:, 2 * A :]
    gg[:, :A] = gur[:, :A]
    gg[:, A:] = last[:, :B]
    ug[:, :A] = gur[:, A : 2 * A]
    ug[:, A:] = last[:, B:]
    put(5, gg, o_gg)
    put(7, ug, o_ug)

    def spread(i):
        for j in range(XH):
            for m in range(2):
                q = j * 2 + m
                gi_cs[m, i * XH + j] = gi_f[i, q * RB : (q + 1) * RB, :].astype(BF)

    loop(0, Z, spread)
    c_start(3, gi_cs.at[o], gi_cr)
    c_copy(3, gi_cs.at[o], gi_cr).wait_recv()

    def pair_sum(i):
        gi_rs[i] = (gi_cs[c, i].astype(FL) + gi_cr[i].astype(FL)).astype(BF)

    loop(0, N, pair_sum)
    tp_rs_start(7, gi_rs, gi_rr)
    gi[...] = tp_rs_sum(7, gi_rs, gi_rr)
    put(6, gi, o_gi)
    for wait in late:
        wait()


def body(
    sizes,
    teacher_in,
    teacher_gate,
    teacher_up,
    teacher_down,
    student_in,
    student_gate,
    student_up,
    student_down,
    projector,
):
    Y, XL, Z, XH = sizes
    G, N = Y * XL, Z * XH
    rb, kt = teacher_in.shape
    ft = teacher_gate.shape[1]
    bt = teacher_down.shape[1]
    ks = student_in.shape[1]
    fs = student_gate.shape[1]
    ds = student_down.shape[1]
    off = projector.shape[2]
    R = rb * N * 2
    rz, rg = R // Z, R // G
    q = ds // (2 * XH)
    proj_t = projector.transpose(1, 2, 0).reshape(-1, projector.shape[0])
    A = fs // 128 * 128
    V = pltpu.VMEM
    D = pltpu.SemaphoreType.DMA
    pair = lambda dt: [
        V((2, R, ds // 2), FL), V((2, R, ds // 2), dt), V((R, ds // 2), dt),
        V((N, rz, q), dt), V((N - 1, rz, q), dt), V((R, ds), dt),
    ]
    scratch = [
        V((kt, ft), BF), V((kt, ft), BF), V((ft, bt), BF), V((bt, ft), BF),
        V((2 * fs, ks), BF), V((fs, ds), BF), V((G * off, ds), BF),
        V((Z, XH, 2, rb, ks), BF), V((rz, ks), FL), V((R, ks), BF),
        V((G, rg, 2 * fs), BF), V((G - 1, rg, 2 * fs), BF), V((rg, 4 * fs - 2 * A), FL),
        V((G, rg, fs), BF),
        *pair(BF),
        V((G, off, R), BF), V((G - 1, off, R), BF), V((G, off, R), BF),
        *pair(BF),
        V((G, rg, fs), BF), V((G - 1, rg, fs), BF), V((G, rg, 2 * fs), BF), V((R, fs), BF), V((R, fs), BF),
        V((Z, rz, ks), FL), V((2, N, rb, ks), BF), V((N, rb, ks), BF), V((N, rb, ks), BF),
        V((N - 1, rb, ks), BF), V((rb, ks), FL),
        V((Z, XH, 2, rb, kt), BF), V((rz, kt), FL), V((R, kt), BF),
        V((G, 2, rg, ft), BF), V((G - 1, 2, rg, ft), BF), V((2, rg, ft), FL), V((G, rg, ft), BF),
        V((2, N, off, R), FL), V((2, N, off, R), BF), V((N, off, R), BF), V((N, off, R), BF),
        V((N - 1, off, R), BF), V((off, R), FL),
        D((9,)), D((2,)), D((8,)), D((8, G)), D((8, G)), D((8, N)), D((8, N)),
        D((8, N)), D((8, N)), D((4,)), D((4,)),
    ]
    S = jax.ShapeDtypeStruct
    x, h, f, rt, fg, gg, ug, gi = pl.pallas_call(
        functools.partial(kernel, sizes),
        out_shape=(
            S((R, ks), BF), S((G, rg, fs), BF), S((R, ds), BF), S((G, off, R), BF),
            S((R, ds), BF), S((R, fs), BF), S((R, fs), BF), S((rb, ks), FL),
        ),
        in_specs=[pl.BlockSpec(memory_space=pl.ANY)] * 9,
        out_specs=tuple([pl.BlockSpec(memory_space=pl.ANY)] * 8),
        scratch_shapes=scratch,
        compiler_params=pltpu.CompilerParams(
            collective_id=0, has_side_effects=True, vmem_limit_bytes=60 * 1024 * 1024
        ),
        name="chain",
    )(
        teacher_in, teacher_gate, teacher_up, teacher_down,
        student_in, student_gate.T, student_up.T, student_down, proj_t,
    )
    h = h.reshape(R, fs)
    grad_projector = dot(rt.reshape(G * off, R), f, 1, 0).reshape(G, off, ds).transpose(2, 0, 1)
    grad_down = dot(h, fg, 0, 0)
    grad_gate = dot(gg, x, 0, 0).T
    grad_up = dot(ug, x, 0, 0).T
    return gi, grad_gate, grad_up, grad_down, grad_projector


def solution(mesh, sizes=(4, 2, 8, 2)):
    torus = Mesh(mesh.devices.reshape(*sizes, 2), AXES)
    in_specs = (
        P(TP, GRP),
        P(GRP, TP),
        P(GRP, TP),
        P(TP, GRP),
        P(TP, GRP),
        P(GRP, TP),
        P(GRP, TP),
        P(TP, GRP),
        P(GRP, None, TP),
    )
    out_specs = (P(TP, GRP), P(GRP, TP), P(GRP, TP), P(TP, GRP), P(GRP, None, TP))
    return jax.shard_map(
        functools.partial(body, sizes), mesh=torus, in_specs=in_specs, out_specs=out_specs, check_vma=False
    )
```

```python
import functools

import jax
import jax.numpy as jnp
from jax import lax
from jax.experimental import pallas as pl
from jax.experimental.pallas import tpu as pltpu
from jax.sharding import Mesh
from jax.sharding import PartitionSpec as P

AXES = ("y", "xl", "z", "xh", "c")
TP = ("z", "xh", "c")
GRP = ("y", "xl")
BF = jnp.bfloat16
FL = jnp.float32


def dot(a, b, ca, cb):
    return lax.dot_general(a, b, (((ca,), (cb,)), ((), ())), preferred_element_type=FL)


def kernel(
    sizes,
    t_in, t_gate, t_up, t_down, s_in, s_gate, s_up, s_down, proj_t,
    o_gp, o_gd, o_gg, o_ug, o_gi,
    w_tg, w_tu, w_td, w_tdt, w_sp, w_sd, w_pt,
    xs, xtmp, x, s2s, s2r, pv, h,
    f_keep, f_cs, f_cr, f_rs, f_rr, f,
    p_s, p_r, rt,
    g_keep, g_cs, g_cr, g_rs, g_rr, fg,
    h_s, h_r, gu, v_gp, v_gd, v_gg, v_ug,
    gi_f, gi_cs, gi_cr, gi_rs, gi_rr, gi,
    ts, ttmp, tx, t2s, t2r, t2a, th,
    tf_keep, tf_cs, tf_cr, tf_rs, tf_rr, tf,
    w_sem, i_sem, o_sem, grp_ss, grp_rs, tp_ss, tp_rs, fw_ss, fw_rs, c_ss, c_rs,
):
    Y, XL, Z, XH = sizes
    G = Y * XL
    N = Z * XH
    y = lax.axis_index("y")
    xl = lax.axis_index("xl")
    z = lax.axis_index("z")
    xh = lax.axis_index("xh")
    c = lax.axis_index("c")
    o = 1 - c
    g = y * XL + xl
    RZ = x.shape[0] // Z
    RB = RZ // (2 * XH)

    def grp_to(k):
        return {"y": lax.rem(y + k // XL, Y), "xl": lax.rem(xl + lax.rem(k, XL), XL)}

    def grp_from(k):
        return lax.rem(y + Y - k // XL, Y) * XL + lax.rem(xl + XL - lax.rem(k, XL), XL)

    def tp_to(k):
        return {"z": lax.rem(z + k // XH, Z), "xh": lax.rem(xh + lax.rem(k, XH), XH)}

    def tp_from(k):
        return lax.rem(z + Z - k // XH, Z), lax.rem(xh + XH - lax.rem(k, XH), XH)

    other = {"c": o}

    def rdma(src, dst, ss, rs, dev):
        return pltpu.make_async_remote_copy(
            src_ref=src, dst_ref=dst, send_sem=ss, recv_sem=rs,
            device_id=dev, device_id_type=pl.DeviceIdType.MESH,
        )

    def loop(lo, hi, body):
        def step(i, carry):
            body(i)
            return carry

        lax.fori_loop(lo, hi, step, 0)

    late = []

    def grp_rs_copy(ph, k, send, recv):
        to = grp_to(k)
        return rdma(
            send.at[to["y"] * XL + to["xl"]], recv.at[k - 1],
            grp_ss.at[ph, k], grp_rs.at[ph, k], to,
        )

    def grp_rs_start(ph, send, recv):
        loop(1, G, lambda k: grp_rs_copy(ph, k, send, recv).start())
        late.append(lambda: loop(1, G, lambda k: grp_rs_copy(ph, k, send, recv).wait_send()))

    def grp_ag_copy(ph, k, buf, at):
        return rdma(buf.at[at(g)], buf.at[at(g)], grp_ss.at[ph, k], grp_rs.at[ph, k], grp_to(k))

    def grp_ag_start(ph, buf, at):
        loop(1, G, lambda k: grp_ag_copy(ph, k, buf, at).start())
        late.append(lambda: loop(1, G, lambda k: grp_ag_copy(ph, k, buf, at).wait_send()))

    def grp_ag_wait(ph, buf, at):
        def one(k):
            src = grp_from(k)
            rdma(
                buf.at[at(src)], buf.at[at(src)], grp_ss.at[ph, k], grp_rs.at[ph, k], grp_to(k)
            ).wait_recv()

        loop(1, G, one)

    def tp_ag_start(ph, buf, at):
        mine = buf.at[at(z, xh, c)]
        loop(1, N, lambda k: rdma(mine, mine, tp_ss.at[ph, k], tp_rs.at[ph, k], tp_to(k)).start())
        rdma(mine, mine, fw_ss.at[ph, 0], fw_rs.at[ph, 0], other).start()
        late.append(
            lambda: loop(
                1, N, lambda k: rdma(mine, mine, tp_ss.at[ph, k], tp_rs.at[ph, k], tp_to(k)).wait_send()
            )
        )
        late.append(
            lambda: loop(
                0, N, lambda k: rdma(mine, mine, fw_ss.at[ph, k], fw_rs.at[ph, k], other).wait_send()
            )
        )

    def tp_ag_forward(ph, buf, at):
        def one(k):
            zz, xx = tp_from(k)
            block = buf.at[at(zz, xx, c)]
            rdma(block, block, tp_ss.at[ph, k], tp_rs.at[ph, k], tp_to(k)).wait_recv()
            rdma(block, block, fw_ss.at[ph, k], fw_rs.at[ph, k], other).start()

        loop(1, N, one)

    def tp_ag_wait(ph, buf, at):
        def one(k):
            zz, xx = tp_from(k)
            block = buf.at[at(zz, xx, o)]
            rdma(block, block, fw_ss.at[ph, k], fw_rs.at[ph, k], other).wait_recv()

        loop(0, N, one)

    def c_copy(ph, src, dst):
        return rdma(src, dst, c_ss.at[ph], c_rs.at[ph], other)

    def c_start(ph, src, dst):
        c_copy(ph, src, dst).start()
        late.append(lambda: c_copy(ph, src, dst).wait_send())

    def tp_rs_copy(ph, k, send, recv):
        to = tp_to(k)
        return rdma(
            send.at[to["z"] * XH + to["xh"]], recv.at[k - 1], tp_ss.at[ph, k], tp_rs.at[ph, k], to
        )

    def tp_rs_start(ph, send, recv):
        loop(1, N, lambda k: tp_rs_copy(ph, k, send, recv).start())
        late.append(lambda: loop(1, N, lambda k: tp_rs_copy(ph, k, send, recv).wait_send()))

    def summed(n, copy, recv, first):
        def step(k, acc):
            copy(k).wait_recv()
            return acc + recv[k - 1].astype(FL)

        return lax.fori_loop(1, n, step, first)

    def tp_rs_sum(ph, send, recv):
        return summed(N, lambda k: tp_rs_copy(ph, k, send, recv), recv, send[z * XH + xh].astype(FL))

    def grp_rs_sum(ph, send, recv):
        return summed(G, lambda k: grp_rs_copy(ph, k, send, recv), recv, send[g].astype(FL))

    def lagged(order, first, second):
        first(order[0])
        for before, now in zip(order, order[1:]):
            first(now)
            second(before)
        second(order[-1])

    Z_ORDER = sorted(range(Z), key=lambda d: min(d, Z - d))
    G_ORDER = sorted(range(G), key=lambda k: min(k // XL, Y - k // XL) + k % XL)

    def tp_arrive(ph, buf, at, dz):
        for k in range(dz * XH, (dz + 1) * XH):
            if k:
                zz, xx = tp_from(k)
                block = buf.at[at(zz, xx, c)]
                rdma(block, block, tp_ss.at[ph, k], tp_rs.at[ph, k], tp_to(k)).wait_recv()
                rdma(block, block, fw_ss.at[ph, k], fw_rs.at[ph, k], other).start()

    def tp_arrived(ph, buf, at, dz):
        for k in range(dz * XH, (dz + 1) * XH):
            zz, xx = tp_from(k)
            block = buf.at[at(zz, xx, o)]
            rdma(block, block, fw_ss.at[ph, k], fw_rs.at[ph, k], other).wait_recv()
        return lax.rem(z + Z - dz, Z)

    def grp_send(ph, i, send, recv):
        k = lax.rem(i // XL + Y - y, Y) * XL + lax.rem(lax.rem(i, XL) + XL - xl, XL)

        @pl.when(k != 0)
        def _():
            grp_rs_copy(ph, k, send, recv).start()

    def grp_sent(ph, send, recv):
        late.append(lambda: loop(1, G, lambda k: grp_rs_copy(ph, k, send, recv).wait_send()))

    def tp_send(ph, i, j, send, recv):
        k = lax.rem(i + Z - z, Z) * XH + lax.rem(j + XH - xh, XH)

        @pl.when(k != 0)
        def _():
            tp_rs_copy(ph, k, send, recv).start()

    def tp_sent(ph, send, recv):
        late.append(lambda: loop(1, N, lambda k: tp_rs_copy(ph, k, send, recv).wait_send()))

    def grp_arrived(ph, buf, k):
        src = grp_from(k)
        if k:
            rdma(
                buf.at[src], buf.at[src], grp_ss.at[ph, k], grp_rs.at[ph, k], grp_to(k)
            ).wait_recv()
        return src

    FS_L = s_gate.shape[0]
    A = FS_L // 128 * 128
    B = FS_L - A
    loads = [
        pltpu.make_async_copy(src, dst, w_sem.at[i])
        for i, (src, dst) in enumerate(
            (
                (s_gate.at[:A], w_sp.at[:A]), (s_up.at[:A], w_sp.at[A : 2 * A]),
                (s_gate.at[A:], w_sp.at[2 * A : A + FS_L]), (s_up.at[A:], w_sp.at[A + FS_L :]),
                (t_gate, w_tg), (t_up, w_tu), (t_down, w_td), (s_down, w_sd), (proj_t, w_pt),
            )
        )
    ]
    in_s = pltpu.make_async_copy(s_in, xs.at[z, xh, c], i_sem.at[0])
    in_t = pltpu.make_async_copy(t_in, ts.at[z, xh, c], i_sem.at[1])
    in_s.start()
    in_t.start()
    for load in loads:
        load.start()

    def put(i, src, dst):
        copy = pltpu.make_async_copy(src, dst, o_sem.at[i])
        copy.start()
        late.append(copy.wait)

    barrier = pltpu.get_barrier_semaphore()

    def greet(dev):
        pl.semaphore_signal(barrier, inc=1, device_id=dev, device_id_type=pl.DeviceIdType.MESH)

    greet(other)
    loop(1, G, lambda k: greet(grp_to(k)))
    loop(1, N, lambda k: greet(tp_to(k)))
    pl.semaphore_wait(barrier, 1 + G - 1 + N - 1)

    def at_block(zz, xx, cc):
        return (zz, xx, cc)

    in_s.wait()
    tp_ag_start(0, xs, at_block)
    in_t.wait()
    tp_ag_start(1, ts, at_block)

    rows_g = x.shape[0] // G
    half = x.shape[0]
    O = p_s.shape[1]

    def compact(blocks, tmp, i):
        for q in range(2 * XH):
            tmp[q * RB : (q + 1) * RB, :] = blocks[i, q // 2, q % 2].astype(FL)
        return tmp[...].astype(BF)

    loads[6].wait()
    FT_L, BT = w_td.shape
    for j in range(BT // 128):
        w_tdt[j * 128 : (j + 1) * 128, :] = w_td[:, j * 128 : (j + 1) * 128].T
    for i in range(6):
        loads[i].wait()

    def s_use(dz):
        i = tp_arrived(0, xs, at_block, dz)
        rows = compact(xs, xtmp, i)
        x[pl.ds(pl.multiple_of(i * RZ, 16), RZ), :] = rows
        s2s[i] = dot(rows, w_sp[...], 1, 1).astype(BF)
        grp_send(0, i, s2s, s2r)

    lagged(Z_ORDER, lambda dz: tp_arrive(0, xs, at_block, dz), s_use)
    grp_sent(0, s2s, s2r)

    def t_use(pair):
        blocks = [tp_arrived(1, ts, at_block, dz) for dz in pair]
        rows = jnp.concatenate([compact(ts, ttmp, i) for i in blocks], axis=0)
        for j, w in enumerate((w_tg, w_tu)):
            out = dot(rows, w[...], 1, 0).astype(BF)
            for n, i in enumerate(blocks):
                t2s[i, j] = out[n * RZ : (n + 1) * RZ]
        for i in blocks:
            grp_send(2, i, t2s, t2r)

    def t_arrive(pair):
        for dz in pair:
            tp_arrive(1, ts, at_block, dz)

    pairs = [Z_ORDER[i : i + 2] for i in range(0, Z, 2)]
    cut = (len(pairs) + 1) // 2
    lagged(pairs[:cut], t_arrive, t_use)

    acc = grp_rs_sum(0, s2s, s2r)
    pv[:, : 2 * A] = acc[:, : 2 * A]
    pv[:, 2 * A : 2 * FS_L] = acc[:, 2 * A :]
    pv[:, 2 * FS_L :] = pltpu.roll(acc[:, 2 * A :], B, 1)

    def pair_values():
        return ((pv[:, :A], pv[:, A : 2 * A], slice(0, A)),
                (pv[:, 2 * A : 2 * FS_L], pv[:, 2 * FS_L :], slice(A, FS_L)))

    for gate, up, cols in pair_values():
        value = (gate * jax.nn.sigmoid(gate) * up).astype(BF)
        h[g, :, cols] = value[:, : cols.stop - cols.start]

    def at_g(i):
        return (i,)

    grp_ag_start(1, h, at_g)
    if pairs[cut:]:
        lagged(pairs[cut:], t_arrive, t_use)
    grp_sent(2, t2s, t2r)

    Q = f.shape[1] // (2 * XH)
    W = f.shape[1] // 2

    def at_tile(zz, xx, cc):
        return (
            pl.ds(pl.multiple_of(zz * RZ, 16), RZ),
            pl.ds(pl.multiple_of((cc * XH + xx) * Q, Q), Q),
        )

    def pair_send(cph, part, i, keep, cs, cr):
        for m in range(2):
            keep[m, i] = part[:, m * W : (m + 1) * W]
            cs[m, i] = part[:, m * W : (m + 1) * W].astype(BF)
        c_copy((cph, i), cs.at[o, i], cr.at[i]).start()

    def pair_sent(cph, cs, cr):
        late.append(lambda: loop(0, Z, lambda i: c_copy((cph, i), cs.at[o, i], cr.at[i]).wait_send()))

    def scatter_send(cph, tph, i, keep, cs, cr, rs, rr):
        c_copy((cph, i), cs.at[o, i], cr.at[i]).wait_recv()
        both = keep[c, i] + cr[i].astype(FL)
        for j in range(XH):
            rs[i * XH + j] = both[:, j * Q : (j + 1) * Q].astype(BF)
            tp_send(tph, i, j, rs, rr)

    loads[7].wait()

    def s4_first(k):
        i = grp_arrived(1, h, k)
        pair_send(0, dot(h[i], w_sd[...], 1, 0), i, f_keep, f_cs, f_cr)

    lagged(
        G_ORDER, s4_first, lambda k: scatter_send(0, 2, grp_from(k), f_keep, f_cs, f_cr, f_rs, f_rr)
    )
    pair_sent(0, f_cs, f_cr)
    tp_sent(2, f_rs, f_rr)

    t2a[...] = t2s[g].astype(FL)

    def t2_add(k):
        grp_rs_copy(2, k, t2s, t2r).wait_recv()
        t2a[...] += t2r[k - 1].astype(FL)

    loop(1, G, t2_add)
    t_pre = t2a[0]
    th[g] = (t_pre * jax.nn.sigmoid(t_pre) * t2a[1]).astype(BF)
    grp_ag_start(3, th, at_g)

    f[at_tile(z, xh, c)] = tp_rs_sum(2, f_rs, f_rr).astype(BF)
    tp_ag_start(3, f, at_tile)

    grp_ag_wait(3, th, at_g)
    thh = th[...].reshape(half, th.shape[2])
    per = BT // Z
    for i in range(Z):
        part = dot(w_tdt[i * per : (i + 1) * per, :], thh, 1, 1)
        for j in range(XH):
            for m in range(2):
                block = part[(j * 2 + m) * O : (j * 2 + m + 1) * O]
                tf_keep[m, i * XH + j] = block
                tf_cs[m, i * XH + j] = block.astype(BF)
    c_start((1, 0), tf_cs.at[o], tf_cr)

    tp_ag_forward(3, f, at_tile)
    c_copy((1, 0), tf_cs.at[o], tf_cr).wait_recv()
    for i in range(N):
        tf_rs[i] = (tf_keep[c, i] + tf_cr[i].astype(FL)).astype(BF)
    tp_rs_start(4, tf_rs, tf_rr)

    tp_ag_wait(3, f, at_tile)

    loads[8].wait()
    p_part = dot(w_pt[...], f[...], 1, 1).astype(BF)
    for i in range(G):
        p_s[i] = p_part[i * O : (i + 1) * O]
    grp_rs_start(4, p_s, p_r)

    projected = grp_rs_sum(4, p_s, p_r)
    tf[...] = tp_rs_sum(4, tf_rs, tf_rr)

    rt[g] = (projected - tf[...].astype(BF).astype(FL)).astype(BF)
    grp_ag_start(5, rt, at_g)
    grp_ag_wait(5, rt, at_g)

    rtt = rt[...].reshape(G * O, half)
    rtn = rtt.T
    for i in range(Z):
        pair_send(2, dot(rtn[i * RZ : (i + 1) * RZ], w_pt[...], 1, 0), i, g_keep, g_cs, g_cr)
    for i in range(Z):
        scatter_send(2, 5, i, g_keep, g_cs, g_cr, g_rs, g_rr)
    pair_sent(2, g_cs, g_cr)
    tp_sent(5, g_rs, g_rr)
    v_gp[...] = dot(rtt, f[...], 1, 0)
    put(0, v_gp, o_gp)
    fg[at_tile(z, xh, c)] = tp_rs_sum(5, g_rs, g_rr).astype(BF)
    tp_ag_start(6, fg, at_tile)

    def s8_use(dz):
        i = tp_arrived(6, fg, at_tile, dz)
        h_s[i] = dot(fg[pl.ds(pl.multiple_of(i * RZ, 16), RZ), :], w_sd[...], 1, 1).astype(BF)
        grp_send(6, i, h_s, h_r)

    lagged(Z_ORDER, lambda dz: tp_arrive(6, fg, at_tile, dz), s8_use)
    grp_sent(6, h_s, h_r)
    v_gd[...] = dot(h[...].reshape(half, FS_L).T, fg[...], 1, 0)
    put(1, v_gd, o_gd)
    hidden_grad = grp_rs_sum(6, h_s, h_r)
    (gate, up, _), (gate_2, up_2, _) = pair_values()

    def pair_grads(grad, gate, up):
        s = jax.nn.sigmoid(gate)
        return grad * up * s * (1.0 + gate * (1.0 - s)), grad * gate * s

    gate_grad, up_grad = pair_grads(hidden_grad[:, :A], gate, up)
    gu[g, :, :A] = gate_grad.astype(BF)
    gu[g, :, A : 2 * A] = up_grad.astype(BF)
    rest = jnp.concatenate([hidden_grad[:, A:], hidden_grad[:, A:]], axis=1)
    gate_grad, up_grad = pair_grads(rest, gate_2, up_2)
    lane = lax.broadcasted_iota(jnp.int32, gate_grad.shape, 1)
    gu[g, :, 2 * A :] = jnp.where(lane < B, gate_grad, pltpu.roll(up_grad, B, 1)).astype(BF)

    grp_ag_start(7, gu, at_g)

    def s10_first(k):
        i = grp_arrived(7, gu, k)
        gi_f[...] = dot(gu[i], w_sp[...], 1, 0)
        for m in range(2):
            for j in range(XH):
                q = j * 2 + m
                gi_cs[m, i, j] = gi_f[q * RB : (q + 1) * RB, :].astype(BF)
        c_copy((3, i), gi_cs.at[o, i], gi_cr.at[i]).start()

    def s10_second(k):
        i = grp_from(k)
        c_copy((3, i), gi_cs.at[o, i], gi_cr.at[i]).wait_recv()
        for j in range(XH):
            gi_rs[i * XH + j] = (gi_cs[c, i, j].astype(FL) + gi_cr[i, j].astype(FL)).astype(BF)
            tp_send(7, i, j, gi_rs, gi_rr)

    lagged(G_ORDER, s10_first, s10_second)
    pair_sent(3, gi_cs, gi_cr)
    tp_sent(7, gi_rs, gi_rr)
    gut = gu[...].reshape(half, 2 * FS_L).T
    v_gg[:A] = dot(gut[:A], x[...], 1, 0)
    v_gg[A:] = dot(gut[2 * A : 2 * A + B], x[...], 1, 0)
    put(2, v_gg, o_gg)
    v_ug[:A] = dot(gut[A : 2 * A], x[...], 1, 0)
    v_ug[A:] = dot(gut[2 * A + B :], x[...], 1, 0)
    put(3, v_ug, o_ug)
    for wait in late:
        wait()
    late.clear()
    gi[...] = tp_rs_sum(7, gi_rs, gi_rr)
    put(4, gi, o_gi)
    for wait in late:
        wait()


def finish(*refs):
    n = len(refs) // 3
    sources, results, held, sem = refs[:n], refs[n : 2 * n], refs[2 * n : 3 * n], refs[-1]
    loads = [pltpu.make_async_copy(sources[i], held[i], sem.at[0, i]) for i in range(n)]
    stores = [pltpu.make_async_copy(held[i], results[i], sem.at[1, i]) for i in range(n)]
    for load in loads:
        load.start()
    for load, store in zip(loads, stores):
        load.wait()
        store.start()
    for store in stores:
        store.wait()


def body(
    sizes,
    teacher_in,
    teacher_gate,
    teacher_up,
    teacher_down,
    student_in,
    student_gate,
    student_up,
    student_down,
    projector,
):
    Y, XL, Z, XH = sizes
    G, N = Y * XL, Z * XH
    rb, kt = teacher_in.shape
    ft = teacher_gate.shape[1]
    bt = teacher_down.shape[1]
    ks = student_in.shape[1]
    fs = student_gate.shape[1]
    ds = student_down.shape[1]
    off = projector.shape[2]
    R = rb * N * 2
    rz, rg = R // Z, R // G
    q = ds // (2 * XH)
    proj_t = projector.transpose(1, 2, 0).reshape(-1, projector.shape[0])
    A = fs // 128 * 128
    V = pltpu.VMEM
    D = pltpu.SemaphoreType.DMA
    pair = lambda dt: [
        V((2, Z, rz, ds // 2), FL), V((2, Z, rz, ds // 2), dt), V((Z, rz, ds // 2), dt),
        V((N, rz, q), dt), V((N - 1, rz, q), dt), V((R, ds), dt),
    ]
    scratch = [
        V((kt, ft), BF), V((kt, ft), BF), V((ft, bt), BF), V((bt, ft), BF),
        V((2 * fs, ks), BF), V((fs, ds), BF), V((G * off, ds), BF),
        V((Z, XH, 2, rb, ks), BF), V((rz, ks), FL), V((R, ks), BF),
        V((G, rg, 2 * fs), BF), V((G - 1, rg, 2 * fs), BF), V((rg, 4 * fs - 2 * A), FL),
        V((G, rg, fs), BF),
        *pair(BF),
        V((G, off, R), BF), V((G - 1, off, R), BF), V((G, off, R), BF),
        *pair(BF),
        V((G, rg, fs), BF), V((G - 1, rg, fs), BF), V((G, rg, 2 * fs), BF), V((G * off, ds), FL), V((fs, ds), FL), V((fs, ks), FL), V((fs, ks), FL),
        V((rz, ks), FL), V((2, Z, XH, rb, ks), BF), V((Z, XH, rb, ks), BF), V((N, rb, ks), BF),
        V((N - 1, rb, ks), BF), V((rb, ks), FL),
        V((Z, XH, 2, rb, kt), BF), V((rz, kt), FL), V((R, kt), BF),
        V((G, 2, rg, ft), BF), V((G - 1, 2, rg, ft), BF), V((2, rg, ft), FL), V((G, rg, ft), BF),
        V((2, N, off, R), FL), V((2, N, off, R), BF), V((N, off, R), BF), V((N, off, R), BF),
        V((N - 1, off, R), BF), V((off, R), FL),
        D((9,)), D((2,)), D((8,)), D((8, G)), D((8, G)), D((8, N)), D((8, N)),
        D((8, N)), D((8, N)), D((4, Z)), D((4, Z)),
    ]
    S = jax.ShapeDtypeStruct
    grads = pl.pallas_call(
        functools.partial(kernel, sizes),
        out_shape=(
            S((G * off, ds), FL), S((fs, ds), FL), S((fs, ks), FL), S((fs, ks), FL), S((rb, ks), FL),
        ),
        in_specs=[pl.BlockSpec(memory_space=pl.ANY)] * 9,
        out_specs=tuple([pl.BlockSpec(memory_space=pl.ANY)] * 5),
        scratch_shapes=scratch,
        compiler_params=pltpu.CompilerParams(
            collective_id=0, has_side_effects=True, vmem_limit_bytes=60 * 1024 * 1024
        ),
        name="chain",
    )(
        teacher_in, teacher_gate, teacher_up, teacher_down,
        student_in, student_gate.T, student_up.T, student_down, proj_t,
    )
    shapes = [(g.shape, g.dtype) for g in grads]
    grad_projector, grad_down, grad_gate, grad_up, grad_input = pl.pallas_call(
        finish,
        out_shape=tuple(S(*shape) for shape in shapes),
        in_specs=[pl.BlockSpec(memory_space=pl.ANY)] * 5,
        out_specs=tuple([pl.BlockSpec(memory_space=pl.ANY)] * 5),
        scratch_shapes=[*(V(*shape) for shape in shapes), D((2, 5))],
        compiler_params=pltpu.CompilerParams(vmem_limit_bytes=60 * 1024 * 1024),
        name="finish",
    )(*grads)
    grad_projector = grad_projector.reshape(G, off, ds).transpose(2, 0, 1)
    return grad_input, grad_gate.T, grad_up.T, grad_down, grad_projector


def solution(mesh, sizes=(4, 2, 8, 2)):
    torus = Mesh(mesh.devices.reshape(*sizes, 2), AXES)
    in_specs = (
        P(TP, GRP),
        P(GRP, TP),
        P(GRP, TP),
        P(TP, GRP),
        P(TP, GRP),
        P(GRP, TP),
        P(GRP, TP),
        P(TP, GRP),
        P(GRP, None, TP),
    )
    out_specs = (P(TP, GRP), P(GRP, TP), P(GRP, TP), P(TP, GRP), P(GRP, None, TP))
    return jax.shard_map(
        functools.partial(body, sizes), mesh=torus, in_specs=in_specs, out_specs=out_specs, check_vma=False
    )
```

```python
import functools

import jax
import jax.numpy as jnp
from jax import lax
from jax.experimental import pallas as pl
from jax.experimental.pallas import tpu as pltpu
from jax.sharding import Mesh
from jax.sharding import PartitionSpec as P

AXES = ("y", "xl", "z", "xh", "c")
TP = ("z", "xh", "c")
GRP = ("y", "xl")
BF = jnp.bfloat16
FL = jnp.float32


def dot(a, b, ca, cb):
    return lax.dot_general(a, b, (((ca,), (cb,)), ((), ())), preferred_element_type=FL)


def kernel(
    sizes,
    t_in, t_gate, t_up, t_down, s_in, s_gate, s_up, s_down, proj_t,
    o_gp, o_gd, o_gg, o_ug, o_gi,
    w_tg, w_tu, w_td, w_tdt, w_sp, w_sd, w_pt,
    xs, xtmp, x, s2s, s2r, pv, h,
    f_keep, f_cs, f_cr, f_rs, f_rr, f,
    p_s, p_r, rt,
    g_keep, g_cs, g_cr, g_rs, g_rr, fg,
    h_s, h_r, gu, v_rt, v_gp, v_gd, v_gg, v_ug,
    gi_f, gi_cs, gi_cr, gi_rs, gi_rr, gi,
    ts, ttmp, tx, t2s, t2r, t2a, th,
    tf_keep, tf_cs, tf_cr, tf_rs, tf_rr, tf,
    w_sem, i_sem, o_sem, grp_ss, grp_rs, tp_ss, tp_rs, fw_ss, fw_rs, c_ss, c_rs,
):
    Y, XL, Z, XH = sizes
    G = Y * XL
    N = Z * XH
    y = lax.axis_index("y")
    xl = lax.axis_index("xl")
    z = lax.axis_index("z")
    xh = lax.axis_index("xh")
    c = lax.axis_index("c")
    o = 1 - c
    g = y * XL + xl
    RZ = x.shape[0] // Z
    RB = RZ // (2 * XH)

    def grp_to(k):
        return {"y": lax.rem(y + k // XL, Y), "xl": lax.rem(xl + lax.rem(k, XL), XL)}

    def grp_from(k):
        return lax.rem(y + Y - k // XL, Y) * XL + lax.rem(xl + XL - lax.rem(k, XL), XL)

    def tp_to(k):
        return {"z": lax.rem(z + k // XH, Z), "xh": lax.rem(xh + lax.rem(k, XH), XH)}

    def tp_from(k):
        return lax.rem(z + Z - k // XH, Z), lax.rem(xh + XH - lax.rem(k, XH), XH)

    other = {"c": o}

    def rdma(src, dst, ss, rs, dev):
        return pltpu.make_async_remote_copy(
            src_ref=src, dst_ref=dst, send_sem=ss, recv_sem=rs,
            device_id=dev, device_id_type=pl.DeviceIdType.MESH,
        )

    def loop(lo, hi, body):
        def step(i, carry):
            body(i)
            return carry

        lax.fori_loop(lo, hi, step, 0)

    late = []

    Z_FAR = sorted(range(Z), key=lambda d: -min(d, Z - d))
    N_FAR = [d * XH + j for d in Z_FAR for j in reversed(range(XH)) if d + j]
    G_FAR = sorted(range(1, G), key=lambda k: -min(k // XL, Y - k // XL) - k % XL)

    def each(order, start):
        for k in order:
            start(k)

    def grp_rs_copy(ph, k, send, recv):
        to = grp_to(k)
        return rdma(
            send.at[to["y"] * XL + to["xl"]], recv.at[k - 1],
            grp_ss.at[ph, k], grp_rs.at[ph, k], to,
        )

    def grp_rs_start(ph, send, recv):
        each(G_FAR, lambda k: grp_rs_copy(ph, k, send, recv).start())
        late.append(lambda: loop(1, G, lambda k: grp_rs_copy(ph, k, send, recv).wait_send()))

    def grp_ag_copy(ph, k, buf, at):
        return rdma(buf.at[at(g)], buf.at[at(g)], grp_ss.at[ph, k], grp_rs.at[ph, k], grp_to(k))

    def grp_ag_start(ph, buf, at, order):
        each(order, lambda k: grp_ag_copy(ph, k, buf, at).start())
        late.append(lambda: loop(1, G, lambda k: grp_ag_copy(ph, k, buf, at).wait_send()))

    def grp_ag_wait(ph, buf, at):
        def one(k):
            src = grp_from(k)
            rdma(
                buf.at[at(src)], buf.at[at(src)], grp_ss.at[ph, k], grp_rs.at[ph, k], grp_to(k)
            ).wait_recv()

        loop(1, G, one)

    def tp_ag_start(ph, buf, at):
        mine = buf.at[at(z, xh, c)]
        loop(1, N, lambda k: rdma(mine, mine, tp_ss.at[ph, k], tp_rs.at[ph, k], tp_to(k)).start())
        rdma(mine, mine, fw_ss.at[ph, 0], fw_rs.at[ph, 0], other).start()
        late.append(
            lambda: loop(
                1, N, lambda k: rdma(mine, mine, tp_ss.at[ph, k], tp_rs.at[ph, k], tp_to(k)).wait_send()
            )
        )
        late.append(
            lambda: loop(
                0, N, lambda k: rdma(mine, mine, fw_ss.at[ph, k], fw_rs.at[ph, k], other).wait_send()
            )
        )

    def tp_ag_forward(ph, buf, at):
        def one(k):
            zz, xx = tp_from(k)
            block = buf.at[at(zz, xx, c)]
            rdma(block, block, tp_ss.at[ph, k], tp_rs.at[ph, k], tp_to(k)).wait_recv()
            rdma(block, block, fw_ss.at[ph, k], fw_rs.at[ph, k], other).start()

        loop(1, N, one)

    def tp_ag_wait(ph, buf, at):
        def one(k):
            zz, xx = tp_from(k)
            block = buf.at[at(zz, xx, o)]
            rdma(block, block, fw_ss.at[ph, k], fw_rs.at[ph, k], other).wait_recv()

        loop(0, N, one)

    def c_copy(ph, src, dst):
        return rdma(src, dst, c_ss.at[ph], c_rs.at[ph], other)

    def c_start(ph, src, dst):
        c_copy(ph, src, dst).start()
        late.append(lambda: c_copy(ph, src, dst).wait_send())

    def tp_rs_copy(ph, k, send, recv):
        to = tp_to(k)
        return rdma(
            send.at[to["z"] * XH + to["xh"]], recv.at[k - 1], tp_ss.at[ph, k], tp_rs.at[ph, k], to
        )

    def tp_rs_start(ph, send, recv):
        each(N_FAR, lambda k: tp_rs_copy(ph, k, send, recv).start())
        late.append(lambda: loop(1, N, lambda k: tp_rs_copy(ph, k, send, recv).wait_send()))

    def summed(n, copy, recv, first):
        def step(k, acc):
            copy(k).wait_recv()
            return acc + recv[k - 1].astype(FL)

        return lax.fori_loop(1, n, step, first)

    def tp_rs_sum(ph, send, recv):
        return summed(N, lambda k: tp_rs_copy(ph, k, send, recv), recv, send[z * XH + xh].astype(FL))

    def grp_rs_sum(ph, send, recv):
        return summed(G, lambda k: grp_rs_copy(ph, k, send, recv), recv, send[g].astype(FL))

    def lagged(order, first, second, lag=1):
        for n in range(len(order) + lag):
            if n < len(order):
                first(order[n])
            if n >= lag:
                second(order[n - lag])

    Z_ORDER = sorted(range(Z), key=lambda d: min(d, Z - d))
    G_ORDER = sorted(range(G), key=lambda k: min(k // XL, Y - k // XL) + k % XL)

    def tp_arrive(ph, buf, at, dz):
        for k in range(dz * XH, (dz + 1) * XH):
            if k:
                zz, xx = tp_from(k)
                block = buf.at[at(zz, xx, c)]
                rdma(block, block, tp_ss.at[ph, k], tp_rs.at[ph, k], tp_to(k)).wait_recv()
                rdma(block, block, fw_ss.at[ph, k], fw_rs.at[ph, k], other).start()

    def tp_arrived(ph, buf, at, dz):
        for k in range(dz * XH, (dz + 1) * XH):
            zz, xx = tp_from(k)
            block = buf.at[at(zz, xx, o)]
            rdma(block, block, fw_ss.at[ph, k], fw_rs.at[ph, k], other).wait_recv()
        return lax.rem(z + Z - dz, Z)

    def grp_send(ph, i, send, recv):
        k = lax.rem(i // XL + Y - y, Y) * XL + lax.rem(lax.rem(i, XL) + XL - xl, XL)

        @pl.when(k != 0)
        def _():
            grp_rs_copy(ph, k, send, recv).start()

    def grp_sent(ph, send, recv):
        late.append(lambda: loop(1, G, lambda k: grp_rs_copy(ph, k, send, recv).wait_send()))

    def tp_send(ph, i, j, send, recv):
        k = lax.rem(i + Z - z, Z) * XH + lax.rem(j + XH - xh, XH)

        @pl.when(k != 0)
        def _():
            tp_rs_copy(ph, k, send, recv).start()

    def tp_sent(ph, send, recv):
        late.append(lambda: loop(1, N, lambda k: tp_rs_copy(ph, k, send, recv).wait_send()))

    def grp_arrived(ph, buf, k):
        src = grp_from(k)
        if k:
            rdma(
                buf.at[src], buf.at[src], grp_ss.at[ph, k], grp_rs.at[ph, k], grp_to(k)
            ).wait_recv()
        return src

    FS_L = s_gate.shape[0]
    A = FS_L // 128 * 128
    B = FS_L - A
    loads = [
        pltpu.make_async_copy(src, dst, w_sem.at[i])
        for i, (src, dst) in enumerate(
            (
                (s_gate.at[:A], w_sp.at[:A]), (s_up.at[:A], w_sp.at[A : 2 * A]),
                (s_gate.at[A:], w_sp.at[2 * A : A + FS_L]), (s_up.at[A:], w_sp.at[A + FS_L :]),
                (t_gate, w_tg), (t_up, w_tu), (t_down, w_td), (s_down, w_sd), (proj_t, w_pt),
            )
        )
    ]
    in_s = pltpu.make_async_copy(s_in, xs.at[z, xh, c], i_sem.at[0])
    in_t = pltpu.make_async_copy(t_in, ts.at[z, xh, c], i_sem.at[1])
    in_s.start()
    in_t.start()
    for load in loads:
        load.start()

    def put(i, src, dst):
        copy = pltpu.make_async_copy(src, dst, o_sem.at[i])
        copy.start()
        late.append(copy.wait)

    barrier = pltpu.get_barrier_semaphore()

    def greet(dev):
        pl.semaphore_signal(barrier, inc=1, device_id=dev, device_id_type=pl.DeviceIdType.MESH)

    greet(other)
    loop(1, G, lambda k: greet(grp_to(k)))
    loop(1, N, lambda k: greet(tp_to(k)))
    pl.semaphore_wait(barrier, 1 + G - 1 + N - 1)

    def at_block(zz, xx, cc):
        return (zz, xx, cc)

    in_s.wait()
    tp_ag_start(0, xs, at_block)
    in_t.wait()
    tp_ag_start(1, ts, at_block)

    rows_g = x.shape[0] // G
    half = x.shape[0]
    O = p_s.shape[1]

    def compact(blocks, tmp, i):
        for q in range(2 * XH):
            tmp[q * RB : (q + 1) * RB, :] = blocks[i, q // 2, q % 2].astype(FL)
        return tmp[...].astype(BF)

    loads[6].wait()
    FT_L, BT = w_td.shape
    for j in range(BT // 128):
        w_tdt[j * 128 : (j + 1) * 128, :] = w_td[:, j * 128 : (j + 1) * 128].T
    for i in range(6):
        loads[i].wait()

    def s_use(dz):
        i = tp_arrived(0, xs, at_block, dz)
        rows = compact(xs, xtmp, i)
        x[pl.ds(pl.multiple_of(i * RZ, 16), RZ), :] = rows
        s2s[i] = dot(rows, w_sp[...], 1, 1).astype(BF)
        grp_send(0, i, s2s, s2r)

    lagged(Z_ORDER, lambda dz: tp_arrive(0, xs, at_block, dz), s_use)
    grp_sent(0, s2s, s2r)

    def t_use(pair):
        blocks = [tp_arrived(1, ts, at_block, dz) for dz in pair]
        rows = jnp.concatenate([compact(ts, ttmp, i) for i in blocks], axis=0)
        for j, w in enumerate((w_tg, w_tu)):
            out = dot(rows, w[...], 1, 0).astype(BF)
            for n, i in enumerate(blocks):
                t2s[i, j] = out[n * RZ : (n + 1) * RZ]
        for i in blocks:
            grp_send(2, i, t2s, t2r)

    def t_arrive(pair):
        for dz in pair:
            tp_arrive(1, ts, at_block, dz)

    pairs = [Z_ORDER[i : i + 2] for i in range(0, Z, 2)]
    cut = (len(pairs) + 1) // 2
    lagged(pairs[:cut], t_arrive, t_use)

    acc = grp_rs_sum(0, s2s, s2r)
    pv[:, : 2 * A] = acc[:, : 2 * A]
    pv[:, 2 * A : 2 * FS_L] = acc[:, 2 * A :]
    pv[:, 2 * FS_L :] = pltpu.roll(acc[:, 2 * A :], B, 1)

    def pair_values():
        return ((pv[:, :A], pv[:, A : 2 * A], slice(0, A)),
                (pv[:, 2 * A : 2 * FS_L], pv[:, 2 * FS_L :], slice(A, FS_L)))

    for gate, up, cols in pair_values():
        value = (gate * jax.nn.sigmoid(gate) * up).astype(BF)
        h[g, :, cols] = value[:, : cols.stop - cols.start]

    def at_g(i):
        return (i,)

    grp_ag_start(1, h, at_g, range(1, G))
    if pairs[cut:]:
        lagged(pairs[cut:], t_arrive, t_use)
    grp_sent(2, t2s, t2r)

    Q = f.shape[1] // (2 * XH)
    W = f.shape[1] // 2

    def at_tile(zz, xx, cc):
        return (
            pl.ds(pl.multiple_of(zz * RZ, 16), RZ),
            pl.ds(pl.multiple_of((cc * XH + xx) * Q, Q), Q),
        )

    def pair_send(cph, part, i, keep, cs, cr):
        for m in range(2):
            keep[m, i] = part[:, m * W : (m + 1) * W]
            cs[m, i] = part[:, m * W : (m + 1) * W].astype(BF)
        c_copy((cph, i), cs.at[o, i], cr.at[i]).start()

    def pair_sent(cph, cs, cr):
        late.append(lambda: loop(0, Z, lambda i: c_copy((cph, i), cs.at[o, i], cr.at[i]).wait_send()))

    def scatter_send(cph, tph, i, keep, cs, cr, rs, rr):
        c_copy((cph, i), cs.at[o, i], cr.at[i]).wait_recv()
        both = keep[c, i] + cr[i].astype(FL)
        for j in range(XH):
            rs[i * XH + j] = both[:, j * Q : (j + 1) * Q].astype(BF)
            tp_send(tph, i, j, rs, rr)

    loads[7].wait()

    def s4_first(k):
        i = grp_arrived(1, h, k)
        pair_send(0, dot(h[i], w_sd[...], 1, 0), i, f_keep, f_cs, f_cr)

    lagged(
        G_ORDER, s4_first, lambda k: scatter_send(0, 2, grp_from(k), f_keep, f_cs, f_cr, f_rs, f_rr)
    )
    pair_sent(0, f_cs, f_cr)
    tp_sent(2, f_rs, f_rr)

    t2a[...] = t2s[g].astype(FL)

    def t2_add(k):
        grp_rs_copy(2, k, t2s, t2r).wait_recv()
        t2a[...] += t2r[k - 1].astype(FL)

    loop(1, G, t2_add)
    t_pre = t2a[0]
    th[g] = (t_pre * jax.nn.sigmoid(t_pre) * t2a[1]).astype(BF)
    grp_ag_start(3, th, at_g, G_FAR)

    f[at_tile(z, xh, c)] = tp_rs_sum(2, f_rs, f_rr).astype(BF)
    tp_ag_start(3, f, at_tile)

    def s5_start():
        tp_ag_wait(3, f, at_tile)
        p_part = dot(w_pt[...], f[...], 1, 1).astype(BF)
        for i in range(G):
            p_s[i] = p_part[i * O : (i + 1) * O]
        grp_rs_start(4, p_s, p_r)

    loads[8].wait()
    grp_ag_wait(3, th, at_g)
    thh = th[...].reshape(half, th.shape[2])
    per = BT // Z

    def t4_pair(i):
        return c_copy((1, i), tf_cs.at[o, i], tf_cr.at[i])

    def t4_first(ds):
        blocks = [lax.rem(z + d, Z) for d in ds]
        rows = [w_tdt[pl.ds(pl.multiple_of(i * per, per), per), :] for i in blocks]
        part = dot(jnp.concatenate(rows, axis=0), thh, 1, 1)
        for n, i in enumerate(blocks):
            for j in range(XH):
                for m in range(2):
                    at = n * per + (j * 2 + m) * O
                    block = part[at : at + O]
                    tf_keep[m, i, j] = block
                    tf_cs[m, i, j] = block.astype(BF)
            t4_pair(i).start()

    def t4_second(ds):
        for d in ds:
            i = lax.rem(z + d, Z)
            t4_pair(i).wait_recv()
            for j in range(XH):
                tf_rs[i * XH + j] = (tf_keep[c, i, j] + tf_cr[i, j].astype(FL)).astype(BF)
                tp_send(4, i, j, tf_rs, tf_rr)

    far = [Z_FAR[i : i + 2] for i in range(0, Z, 2)]
    mid = max(1, len(far) // 2)
    for n, ds in enumerate(far[:mid]):
        t4_first(ds)
        if n:
            t4_second(far[n - 1])
    tp_ag_forward(3, f, at_tile)
    for n in range(mid, len(far)):
        t4_second(far[n - 1])
        if n == len(far) - 1:
            s5_start()
        t4_first(far[n])
    if mid == len(far):
        s5_start()
    t4_second(far[-1])
    pair_sent(1, tf_cs, tf_cr)
    tp_sent(4, tf_rs, tf_rr)

    projected = grp_rs_sum(4, p_s, p_r)
    tf[...] = tp_rs_sum(4, tf_rs, tf_rr)

    rt[g] = (projected - tf[...].astype(BF).astype(FL)).astype(BF)
    grp_ag_start(5, rt, at_g, G_FAR)
    grp_ag_wait(5, rt, at_g)

    rtt = rt[...].reshape(G * O, half)
    v_rt[...] = rtt.T

    def s7_first(d):
        i = lax.rem(z + d, Z)
        rows = v_rt[pl.ds(pl.multiple_of(i * RZ, 16), RZ), :]
        pair_send(2, dot(rows, w_pt[...], 1, 0), i, g_keep, g_cs, g_cr)

    lagged(
        Z_FAR,
        s7_first,
        lambda d: scatter_send(2, 5, lax.rem(z + d, Z), g_keep, g_cs, g_cr, g_rs, g_rr),
        lag=min(3, Z),
    )
    pair_sent(2, g_cs, g_cr)
    tp_sent(5, g_rs, g_rr)
    v_gp[...] = dot(rtt, f[...], 1, 0)
    put(0, v_gp, o_gp)
    fg[at_tile(z, xh, c)] = tp_rs_sum(5, g_rs, g_rr).astype(BF)
    tp_ag_start(6, fg, at_tile)

    def s8_use(dz):
        i = tp_arrived(6, fg, at_tile, dz)
        h_s[i] = dot(fg[pl.ds(pl.multiple_of(i * RZ, 16), RZ), :], w_sd[...], 1, 1).astype(BF)
        grp_send(6, i, h_s, h_r)

    lagged(Z_ORDER, lambda dz: tp_arrive(6, fg, at_tile, dz), s8_use)
    grp_sent(6, h_s, h_r)
    v_gd[...] = dot(h[...].reshape(half, FS_L).T, fg[...], 1, 0)
    put(1, v_gd, o_gd)
    hidden_grad = grp_rs_sum(6, h_s, h_r)
    (gate, up, _), (gate_2, up_2, _) = pair_values()

    def pair_grads(grad, gate, up):
        s = jax.nn.sigmoid(gate)
        return grad * up * s * (1.0 + gate * (1.0 - s)), grad * gate * s

    gate_grad, up_grad = pair_grads(hidden_grad[:, :A], gate, up)
    gu[g, :, :A] = gate_grad.astype(BF)
    gu[g, :, A : 2 * A] = up_grad.astype(BF)
    rest = jnp.concatenate([hidden_grad[:, A:], hidden_grad[:, A:]], axis=1)
    gate_grad, up_grad = pair_grads(rest, gate_2, up_2)
    lane = lax.broadcasted_iota(jnp.int32, gate_grad.shape, 1)
    gu[g, :, 2 * A :] = jnp.where(lane < B, gate_grad, pltpu.roll(up_grad, B, 1)).astype(BF)

    grp_ag_start(7, gu, at_g, range(1, G))

    def s10_first(k):
        i = grp_arrived(7, gu, k)
        gi_f[...] = dot(gu[i], w_sp[...], 1, 0)
        for m in range(2):
            for j in range(XH):
                q = j * 2 + m
                gi_cs[m, i, j] = gi_f[q * RB : (q + 1) * RB, :].astype(BF)
        c_copy((3, i), gi_cs.at[o, i], gi_cr.at[i]).start()

    def s10_second(k):
        i = grp_from(k)
        c_copy((3, i), gi_cs.at[o, i], gi_cr.at[i]).wait_recv()
        for j in range(XH):
            gi_rs[i * XH + j] = (gi_cs[c, i, j].astype(FL) + gi_cr[i, j].astype(FL)).astype(BF)
            tp_send(7, i, j, gi_rs, gi_rr)

    lagged(G_ORDER, s10_first, s10_second)
    pair_sent(3, gi_cs, gi_cr)
    tp_sent(7, gi_rs, gi_rr)
    gut = gu[...].reshape(half, 2 * FS_L).T
    v_gg[:A] = dot(gut[:A], x[...], 1, 0)
    v_gg[A:] = dot(gut[2 * A : 2 * A + B], x[...], 1, 0)
    put(2, v_gg, o_gg)
    v_ug[:A] = dot(gut[A : 2 * A], x[...], 1, 0)
    v_ug[A:] = dot(gut[2 * A + B :], x[...], 1, 0)
    put(3, v_ug, o_ug)
    for wait in late:
        wait()
    late.clear()
    gi[...] = tp_rs_sum(7, gi_rs, gi_rr)
    put(4, gi, o_gi)
    for wait in late:
        wait()


def finish(*refs):
    n = len(refs) // 3
    sources, results, held, sem = refs[:n], refs[n : 2 * n], refs[2 * n : 3 * n], refs[-1]
    loads = [pltpu.make_async_copy(sources[i], held[i], sem.at[0, i]) for i in range(n)]
    stores = [pltpu.make_async_copy(held[i], results[i], sem.at[1, i]) for i in range(n)]
    for load in loads:
        load.start()
    for load, store in zip(loads, stores):
        load.wait()
        store.start()
    for store in stores:
        store.wait()


def body(
    sizes,
    teacher_in,
    teacher_gate,
    teacher_up,
    teacher_down,
    student_in,
    student_gate,
    student_up,
    student_down,
    projector,
):
    Y, XL, Z, XH = sizes
    G, N = Y * XL, Z * XH
    rb, kt = teacher_in.shape
    ft = teacher_gate.shape[1]
    bt = teacher_down.shape[1]
    ks = student_in.shape[1]
    fs = student_gate.shape[1]
    ds = student_down.shape[1]
    off = projector.shape[2]
    R = rb * N * 2
    rz, rg = R // Z, R // G
    q = ds // (2 * XH)
    proj_t = projector.transpose(1, 2, 0).reshape(-1, projector.shape[0])
    A = fs // 128 * 128
    V = pltpu.VMEM
    D = pltpu.SemaphoreType.DMA
    pair = lambda dt: [
        V((2, Z, rz, ds // 2), FL), V((2, Z, rz, ds // 2), dt), V((Z, rz, ds // 2), dt),
        V((N, rz, q), dt), V((N - 1, rz, q), dt), V((R, ds), dt),
    ]
    scratch = [
        V((kt, ft), BF), V((kt, ft), BF), V((ft, bt), BF), V((bt, ft), BF),
        V((2 * fs, ks), BF), V((fs, ds), BF), V((G * off, ds), BF),
        V((Z, XH, 2, rb, ks), BF), V((rz, ks), FL), V((R, ks), BF),
        V((G, rg, 2 * fs), BF), V((G - 1, rg, 2 * fs), BF), V((rg, 4 * fs - 2 * A), FL),
        V((G, rg, fs), BF),
        *pair(BF),
        V((G, off, R), BF), V((G - 1, off, R), BF), V((G, off, R), BF),
        *pair(BF),
        V((G, rg, fs), BF), V((G - 1, rg, fs), BF), V((G, rg, 2 * fs), BF), V((R, G * off), BF), V((G * off, ds), FL), V((fs, ds), FL), V((fs, ks), FL), V((fs, ks), FL),
        V((rz, ks), FL), V((2, Z, XH, rb, ks), BF), V((Z, XH, rb, ks), BF), V((N, rb, ks), BF),
        V((N - 1, rb, ks), BF), V((rb, ks), FL),
        V((Z, XH, 2, rb, kt), BF), V((rz, kt), FL), V((R, kt), BF),
        V((G, 2, rg, ft), BF), V((G - 1, 2, rg, ft), BF), V((2, rg, ft), FL), V((G, rg, ft), BF),
        V((2, Z, XH, off, R), FL), V((2, Z, XH, off, R), BF), V((Z, XH, off, R), BF), V((N, off, R), BF),
        V((N - 1, off, R), BF), V((off, R), FL),
        D((9,)), D((2,)), D((8,)), D((8, G)), D((8, G)), D((8, N)), D((8, N)),
        D((8, N)), D((8, N)), D((4, Z)), D((4, Z)),
    ]
    S = jax.ShapeDtypeStruct
    grads = pl.pallas_call(
        functools.partial(kernel, sizes),
        out_shape=(
            S((G * off, ds), FL), S((fs, ds), FL), S((fs, ks), FL), S((fs, ks), FL), S((rb, ks), FL),
        ),
        in_specs=[pl.BlockSpec(memory_space=pl.ANY)] * 9,
        out_specs=tuple([pl.BlockSpec(memory_space=pl.ANY)] * 5),
        scratch_shapes=scratch,
        compiler_params=pltpu.CompilerParams(
            collective_id=0, has_side_effects=True, vmem_limit_bytes=60 * 1024 * 1024
        ),
        name="chain",
    )(
        teacher_in, teacher_gate, teacher_up, teacher_down,
        student_in, student_gate.T, student_up.T, student_down, proj_t,
    )
    shapes = [(g.shape, g.dtype) for g in grads]
    grad_projector, grad_down, grad_gate, grad_up, grad_input = pl.pallas_call(
        finish,
        out_shape=tuple(S(*shape) for shape in shapes),
        in_specs=[pl.BlockSpec(memory_space=pl.ANY)] * 5,
        out_specs=tuple([pl.BlockSpec(memory_space=pl.ANY)] * 5),
        scratch_shapes=[*(V(*shape) for shape in shapes), D((2, 5))],
        compiler_params=pltpu.CompilerParams(vmem_limit_bytes=60 * 1024 * 1024),
        name="finish",
    )(*grads)
    grad_projector = grad_projector.reshape(G, off, ds).transpose(2, 0, 1)
    return grad_input, grad_gate.T, grad_up.T, grad_down, grad_projector


def solution(mesh, sizes=(4, 2, 8, 2)):
    torus = Mesh(mesh.devices.reshape(*sizes, 2), AXES)
    in_specs = (
        P(TP, GRP),
        P(GRP, TP),
        P(GRP, TP),
        P(TP, GRP),
        P(TP, GRP),
        P(GRP, TP),
        P(GRP, TP),
        P(TP, GRP),
        P(GRP, None, TP),
    )
    out_specs = (P(TP, GRP), P(GRP, TP), P(GRP, TP), P(TP, GRP), P(GRP, None, TP))
    return jax.shard_map(
        functools.partial(body, sizes), mesh=torus, in_specs=in_specs, out_specs=out_specs, check_vma=False
    )
```

```python
import functools

import jax
import jax.numpy as jnp
from jax import lax
from jax.experimental import pallas as pl
from jax.experimental.pallas import tpu as pltpu
from jax.sharding import Mesh
from jax.sharding import PartitionSpec as P

AXES = ("y", "xl", "z", "xh", "c")
TP = ("z", "xh", "c")
GRP = ("y", "xl")
BF = jnp.bfloat16
FL = jnp.float32


def dot(a, b, ca, cb):
    return lax.dot_general(a, b, (((ca,), (cb,)), ((), ())), preferred_element_type=FL)


def kernel(
    sizes,
    t_in, t_gate, t_up, t_down, s_in, s_gate, s_up, s_down, proj_t,
    o_gp, o_gd, o_gg, o_ug, o_gi,
    w_tg, w_tu, w_td, w_tdt, w_sp, w_sd, w_pt,
    xs, xtmp, x, s2s, s2r, pv, h,
    f_keep, f_cs, f_cr, f_rs, f_rr, f,
    p_s, p_r, rt,
    g_keep, g_cs, g_cr, g_rs, g_rr, fg,
    h_s, h_r, gu, v_rt, v_gp, v_gd, v_gg, v_ug,
    gi_f, gi_cs, gi_cr, gi_rs, gi_rr, gi,
    ts, ttmp, tx, t2s, t2r, t2a, th,
    tf_keep, tf_cs, tf_cr, tf_rs, tf_rr, tf,
    w_sem, i_sem, o_sem, grp_ss, grp_rs, tp_ss, tp_rs, fw_ss, fw_rs, c_ss, c_rs,
):
    Y, XL, Z, XH = sizes
    G = Y * XL
    N = Z * XH
    y = lax.axis_index("y")
    xl = lax.axis_index("xl")
    z = lax.axis_index("z")
    xh = lax.axis_index("xh")
    c = lax.axis_index("c")
    o = 1 - c
    g = y * XL + xl
    RZ = x.shape[0] // Z
    RB = RZ // (2 * XH)

    def grp_to(k):
        return {"y": lax.rem(y + k // XL, Y), "xl": lax.rem(xl + lax.rem(k, XL), XL)}

    def grp_from(k):
        return lax.rem(y + Y - k // XL, Y) * XL + lax.rem(xl + XL - lax.rem(k, XL), XL)

    def tp_to(k):
        return {"z": lax.rem(z + k // XH, Z), "xh": lax.rem(xh + lax.rem(k, XH), XH)}

    def tp_from(k):
        return lax.rem(z + Z - k // XH, Z), lax.rem(xh + XH - lax.rem(k, XH), XH)

    other = {"c": o}

    def rdma(src, dst, ss, rs, dev):
        return pltpu.make_async_remote_copy(
            src_ref=src, dst_ref=dst, send_sem=ss, recv_sem=rs,
            device_id=dev, device_id_type=pl.DeviceIdType.MESH,
        )

    def loop(lo, hi, body):
        def step(i, carry):
            body(i)
            return carry

        lax.fori_loop(lo, hi, step, 0)

    late = []

    Z_FAR = sorted(range(Z), key=lambda d: -min(d, Z - d))
    N_FAR = [d * XH + j for d in Z_FAR for j in reversed(range(XH)) if d + j]
    G_FAR = sorted(range(1, G), key=lambda k: -min(k // XL, Y - k // XL) - k % XL)

    def each(order, start):
        for k in order:
            start(k)

    def grp_rs_copy(ph, k, send, recv):
        to = grp_to(k)
        return rdma(
            send.at[to["y"] * XL + to["xl"]], recv.at[k - 1],
            grp_ss.at[ph, k], grp_rs.at[ph, k], to,
        )

    def grp_rs_start(ph, send, recv):
        each(G_FAR, lambda k: grp_rs_copy(ph, k, send, recv).start())
        late.append(lambda: loop(1, G, lambda k: grp_rs_copy(ph, k, send, recv).wait_send()))

    def grp_ag_copy(ph, k, buf, at):
        return rdma(buf.at[at(g)], buf.at[at(g)], grp_ss.at[ph, k], grp_rs.at[ph, k], grp_to(k))

    def grp_ag_start(ph, buf, at, order):
        each(order, lambda k: grp_ag_copy(ph, k, buf, at).start())
        late.append(lambda: loop(1, G, lambda k: grp_ag_copy(ph, k, buf, at).wait_send()))

    def grp_ag_wait(ph, buf, at):
        def one(k):
            src = grp_from(k)
            rdma(
                buf.at[at(src)], buf.at[at(src)], grp_ss.at[ph, k], grp_rs.at[ph, k], grp_to(k)
            ).wait_recv()

        loop(1, G, one)

    def tp_ag_start(ph, buf, at):
        mine = buf.at[at(z, xh, c)]
        each(N_FAR[::-1], lambda k: rdma(mine, mine, tp_ss.at[ph, k], tp_rs.at[ph, k], tp_to(k)).start())
        rdma(mine, mine, fw_ss.at[ph, 0], fw_rs.at[ph, 0], other).start()
        late.append(
            lambda: loop(
                1, N, lambda k: rdma(mine, mine, tp_ss.at[ph, k], tp_rs.at[ph, k], tp_to(k)).wait_send()
            )
        )
        late.append(
            lambda: loop(
                0, N, lambda k: rdma(mine, mine, fw_ss.at[ph, k], fw_rs.at[ph, k], other).wait_send()
            )
        )

    def tp_ag_forward(ph, buf, at):
        def one(k):
            zz, xx = tp_from(k)
            block = buf.at[at(zz, xx, c)]
            rdma(block, block, tp_ss.at[ph, k], tp_rs.at[ph, k], tp_to(k)).wait_recv()
            rdma(block, block, fw_ss.at[ph, k], fw_rs.at[ph, k], other).start()

        loop(1, N, one)

    def tp_ag_wait(ph, buf, at):
        def one(k):
            zz, xx = tp_from(k)
            block = buf.at[at(zz, xx, o)]
            rdma(block, block, fw_ss.at[ph, k], fw_rs.at[ph, k], other).wait_recv()

        loop(0, N, one)

    def c_copy(ph, src, dst):
        return rdma(src, dst, c_ss.at[ph], c_rs.at[ph], other)

    def c_start(ph, src, dst):
        c_copy(ph, src, dst).start()
        late.append(lambda: c_copy(ph, src, dst).wait_send())

    def tp_rs_copy(ph, k, send, recv):
        to = tp_to(k)
        return rdma(
            send.at[to["z"] * XH + to["xh"]], recv.at[k - 1], tp_ss.at[ph, k], tp_rs.at[ph, k], to
        )

    def tp_rs_start(ph, send, recv):
        each(N_FAR, lambda k: tp_rs_copy(ph, k, send, recv).start())
        late.append(lambda: loop(1, N, lambda k: tp_rs_copy(ph, k, send, recv).wait_send()))

    def summed(n, copy, recv, first):
        def step(k, acc):
            copy(k).wait_recv()
            return acc + recv[k - 1].astype(FL)

        return lax.fori_loop(1, n, step, first)

    def tp_rs_sum(ph, send, recv):
        return summed(N, lambda k: tp_rs_copy(ph, k, send, recv), recv, send[z * XH + xh].astype(FL))

    def grp_rs_sum(ph, send, recv):
        return summed(G, lambda k: grp_rs_copy(ph, k, send, recv), recv, send[g].astype(FL))

    def lagged(order, first, second, lag=1):
        for n in range(len(order) + lag):
            if n < len(order):
                first(order[n])
            if n >= lag:
                second(order[n - lag])

    Z_ORDER = sorted(range(Z), key=lambda d: min(d, Z - d))
    G_ORDER = sorted(range(G), key=lambda k: min(k // XL, Y - k // XL) + k % XL)

    def tp_arrive(ph, buf, at, dz):
        for k in range(dz * XH, (dz + 1) * XH):
            if k:
                zz, xx = tp_from(k)
                block = buf.at[at(zz, xx, c)]
                rdma(block, block, tp_ss.at[ph, k], tp_rs.at[ph, k], tp_to(k)).wait_recv()
                rdma(block, block, fw_ss.at[ph, k], fw_rs.at[ph, k], other).start()

    def tp_arrived(ph, buf, at, dz):
        for k in range(dz * XH, (dz + 1) * XH):
            zz, xx = tp_from(k)
            block = buf.at[at(zz, xx, o)]
            rdma(block, block, fw_ss.at[ph, k], fw_rs.at[ph, k], other).wait_recv()
        return lax.rem(z + Z - dz, Z)

    def grp_send(ph, i, send, recv):
        k = lax.rem(i // XL + Y - y, Y) * XL + lax.rem(lax.rem(i, XL) + XL - xl, XL)

        @pl.when(k != 0)
        def _():
            grp_rs_copy(ph, k, send, recv).start()

    def grp_sent(ph, send, recv):
        late.append(lambda: loop(1, G, lambda k: grp_rs_copy(ph, k, send, recv).wait_send()))

    def tp_send(ph, i, j, send, recv):
        k = lax.rem(i + Z - z, Z) * XH + lax.rem(j + XH - xh, XH)

        @pl.when(k != 0)
        def _():
            tp_rs_copy(ph, k, send, recv).start()

    def tp_sent(ph, send, recv):
        late.append(lambda: loop(1, N, lambda k: tp_rs_copy(ph, k, send, recv).wait_send()))

    def grp_arrived(ph, buf, k):
        src = grp_from(k)
        if k:
            rdma(
                buf.at[src], buf.at[src], grp_ss.at[ph, k], grp_rs.at[ph, k], grp_to(k)
            ).wait_recv()
        return src

    FS_L = s_gate.shape[0]
    A = FS_L // 128 * 128
    B = FS_L - A
    loads = [
        pltpu.make_async_copy(src, dst, w_sem.at[i])
        for i, (src, dst) in enumerate(
            (
                (s_gate.at[:A], w_sp.at[:A]), (s_up.at[:A], w_sp.at[A : 2 * A]),
                (s_gate.at[A:], w_sp.at[2 * A : A + FS_L]), (s_up.at[A:], w_sp.at[A + FS_L :]),
                (t_gate, w_tg), (t_up, w_tu), (t_down, w_td), (s_down, w_sd), (proj_t, w_pt),
            )
        )
    ]
    in_s = pltpu.make_async_copy(s_in, xs.at[z, xh, c], i_sem.at[0])
    in_t = pltpu.make_async_copy(t_in, ts.at[z, xh, c], i_sem.at[1])
    in_s.start()
    in_t.start()
    for load in loads:
        load.start()

    def put(i, src, dst):
        copy = pltpu.make_async_copy(src, dst, o_sem.at[i])
        copy.start()
        late.append(copy.wait)

    barrier = pltpu.get_barrier_semaphore()

    def greet(dev):
        pl.semaphore_signal(barrier, inc=1, device_id=dev, device_id_type=pl.DeviceIdType.MESH)

    greet(other)
    loop(1, G, lambda k: greet(grp_to(k)))
    loop(1, N, lambda k: greet(tp_to(k)))
    pl.semaphore_wait(barrier, 1 + G - 1 + N - 1)

    def at_block(zz, xx, cc):
        return (zz, xx, cc)

    in_s.wait()
    tp_ag_start(0, xs, at_block)
    in_t.wait()
    tp_ag_start(1, ts, at_block)

    rows_g = x.shape[0] // G
    half = x.shape[0]
    O = p_s.shape[1]

    def compact(blocks, tmp, i):
        for q in range(2 * XH):
            tmp[q * RB : (q + 1) * RB, :] = blocks[i, q // 2, q % 2].astype(FL)
        return tmp[...].astype(BF)

    loads[6].wait()
    FT_L, BT = w_td.shape
    for j in range(BT // 128):
        w_tdt[j * 128 : (j + 1) * 128, :] = w_td[:, j * 128 : (j + 1) * 128].T
    for i in range(6):
        loads[i].wait()

    def s_use(dz):
        i = tp_arrived(0, xs, at_block, dz)
        rows = compact(xs, xtmp, i)
        x[pl.ds(pl.multiple_of(i * RZ, 16), RZ), :] = rows
        s2s[i] = dot(rows, w_sp[...], 1, 1).astype(BF)
        grp_send(0, i, s2s, s2r)

    lagged(Z_ORDER, lambda dz: tp_arrive(0, xs, at_block, dz), s_use)
    grp_sent(0, s2s, s2r)

    def t_use(pair):
        blocks = [tp_arrived(1, ts, at_block, dz) for dz in pair]
        rows = jnp.concatenate([compact(ts, ttmp, i) for i in blocks], axis=0)
        for j, w in enumerate((w_tg, w_tu)):
            out = dot(rows, w[...], 1, 0).astype(BF)
            for n, i in enumerate(blocks):
                t2s[i, j] = out[n * RZ : (n + 1) * RZ]
        for i in blocks:
            grp_send(2, i, t2s, t2r)

    def t_arrive(pair):
        for dz in pair:
            tp_arrive(1, ts, at_block, dz)

    pairs = [Z_ORDER[i : i + 2] for i in range(0, Z, 2)]
    cut = (len(pairs) + 1) // 2
    lagged(pairs[:cut], t_arrive, t_use)

    acc = grp_rs_sum(0, s2s, s2r)
    pv[:, : 2 * A] = acc[:, : 2 * A]
    pv[:, 2 * A : 2 * FS_L] = acc[:, 2 * A :]
    pv[:, 2 * FS_L :] = pltpu.roll(acc[:, 2 * A :], B, 1)

    def pair_values():
        return ((pv[:, :A], pv[:, A : 2 * A], slice(0, A)),
                (pv[:, 2 * A : 2 * FS_L], pv[:, 2 * FS_L :], slice(A, FS_L)))

    for gate, up, cols in pair_values():
        value = (gate * jax.nn.sigmoid(gate) * up).astype(BF)
        h[g, :, cols] = value[:, : cols.stop - cols.start]

    def at_g(i):
        return (i,)

    grp_ag_start(1, h, at_g, G_ORDER[1:])
    if pairs[cut:]:
        lagged(pairs[cut:], t_arrive, t_use)
    grp_sent(2, t2s, t2r)

    Q = f.shape[1] // (2 * XH)
    W = f.shape[1] // 2

    def at_tile(zz, xx, cc):
        return (
            pl.ds(pl.multiple_of(zz * RZ, 16), RZ),
            pl.ds(pl.multiple_of((cc * XH + xx) * Q, Q), Q),
        )

    def pair_send(cph, part, i, keep, cs, cr):
        for m in range(2):
            keep[m, i] = part[:, m * W : (m + 1) * W]
            cs[m, i] = part[:, m * W : (m + 1) * W].astype(BF)
        c_copy((cph, i), cs.at[o, i], cr.at[i]).start()

    def pair_sent(cph, cs, cr):
        late.append(lambda: loop(0, Z, lambda i: c_copy((cph, i), cs.at[o, i], cr.at[i]).wait_send()))

    def scatter_send(cph, tph, i, keep, cs, cr, rs, rr):
        c_copy((cph, i), cs.at[o, i], cr.at[i]).wait_recv()
        both = keep[c, i] + cr[i].astype(FL)
        for j in range(XH):
            rs[i * XH + j] = both[:, j * Q : (j + 1) * Q].astype(BF)
            tp_send(tph, i, j, rs, rr)

    loads[7].wait()

    def s4_first(k):
        i = grp_arrived(1, h, k)
        pair_send(0, dot(h[i], w_sd[...], 1, 0), i, f_keep, f_cs, f_cr)

    lagged(
        G_ORDER, s4_first, lambda k: scatter_send(0, 2, grp_from(k), f_keep, f_cs, f_cr, f_rs, f_rr)
    )
    pair_sent(0, f_cs, f_cr)
    tp_sent(2, f_rs, f_rr)

    t2a[...] = t2s[g].astype(FL)

    def t2_add(k):
        grp_rs_copy(2, k, t2s, t2r).wait_recv()
        t2a[...] += t2r[k - 1].astype(FL)

    loop(1, G, t2_add)
    t_pre = t2a[0]
    th[g] = (t_pre * jax.nn.sigmoid(t_pre) * t2a[1]).astype(BF)
    grp_ag_start(3, th, at_g, G_FAR)

    f[at_tile(z, xh, c)] = tp_rs_sum(2, f_rs, f_rr).astype(BF)
    tp_ag_start(3, f, at_tile)

    def s5_start():
        tp_ag_wait(3, f, at_tile)
        p_part = dot(w_pt[...], f[...], 1, 1).astype(BF)
        for i in range(G):
            p_s[i] = p_part[i * O : (i + 1) * O]
        grp_rs_start(4, p_s, p_r)

    loads[8].wait()
    grp_ag_wait(3, th, at_g)
    thh = th[...].reshape(half, th.shape[2])
    per = BT // Z

    def t4_pair(i):
        return c_copy((1, i), tf_cs.at[o, i], tf_cr.at[i])

    def t4_first(ds):
        blocks = [lax.rem(z + d, Z) for d in ds]
        rows = [w_tdt[pl.ds(pl.multiple_of(i * per, per), per), :] for i in blocks]
        part = dot(jnp.concatenate(rows, axis=0), thh, 1, 1)
        for n, i in enumerate(blocks):
            for j in range(XH):
                for m in range(2):
                    at = n * per + (j * 2 + m) * O
                    block = part[at : at + O]
                    tf_keep[m, i, j] = block
                    tf_cs[m, i, j] = block.astype(BF)
            t4_pair(i).start()

    def t4_second(ds):
        for d in ds:
            i = lax.rem(z + d, Z)
            t4_pair(i).wait_recv()
            for j in range(XH):
                tf_rs[i * XH + j] = (tf_keep[c, i, j] + tf_cr[i, j].astype(FL)).astype(BF)
                tp_send(4, i, j, tf_rs, tf_rr)

    far = [Z_FAR[i : i + 2] for i in range(0, Z, 2)]
    mid = max(1, len(far) // 2)
    for n, ds in enumerate(far[:mid]):
        t4_first(ds)
        if n:
            t4_second(far[n - 1])
    tp_ag_forward(3, f, at_tile)
    for n in range(mid, len(far)):
        t4_second(far[n - 1])
        if n == len(far) - 1:
            s5_start()
        t4_first(far[n])
    if mid == len(far):
        s5_start()
    t4_second(far[-1])
    pair_sent(1, tf_cs, tf_cr)
    tp_sent(4, tf_rs, tf_rr)

    projected = grp_rs_sum(4, p_s, p_r)
    tf[...] = tp_rs_sum(4, tf_rs, tf_rr)

    rt[g] = (projected - tf[...].astype(BF).astype(FL)).astype(BF)
    grp_ag_start(5, rt, at_g, G_FAR)
    grp_ag_wait(5, rt, at_g)

    rtt = rt[...].reshape(G * O, half)
    v_rt[...] = rtt.T

    def s7_first(d):
        i = lax.rem(z + d, Z)
        rows = v_rt[pl.ds(pl.multiple_of(i * RZ, 16), RZ), :]
        pair_send(2, dot(rows, w_pt[...], 1, 0), i, g_keep, g_cs, g_cr)

    lagged(
        Z_FAR,
        s7_first,
        lambda d: scatter_send(2, 5, lax.rem(z + d, Z), g_keep, g_cs, g_cr, g_rs, g_rr),
        lag=min(3, Z),
    )
    pair_sent(2, g_cs, g_cr)
    tp_sent(5, g_rs, g_rr)
    v_gp[...] = dot(rtt, f[...], 1, 0)
    put(0, v_gp, o_gp)
    fg[at_tile(z, xh, c)] = tp_rs_sum(5, g_rs, g_rr).astype(BF)
    tp_ag_start(6, fg, at_tile)

    def s8_use(dz):
        i = tp_arrived(6, fg, at_tile, dz)
        h_s[i] = dot(fg[pl.ds(pl.multiple_of(i * RZ, 16), RZ), :], w_sd[...], 1, 1).astype(BF)
        grp_send(6, i, h_s, h_r)

    lagged(Z_ORDER, lambda dz: tp_arrive(6, fg, at_tile, dz), s8_use)
    grp_sent(6, h_s, h_r)
    v_gd[...] = dot(h[...].reshape(half, FS_L).T, fg[...], 1, 0)
    put(1, v_gd, o_gd)
    hidden_grad = grp_rs_sum(6, h_s, h_r)
    (gate, up, _), (gate_2, up_2, _) = pair_values()

    def pair_grads(grad, gate, up):
        s = jax.nn.sigmoid(gate)
        return grad * up * s * (1.0 + gate * (1.0 - s)), grad * gate * s

    gate_grad, up_grad = pair_grads(hidden_grad[:, :A], gate, up)
    gu[g, :, :A] = gate_grad.astype(BF)
    gu[g, :, A : 2 * A] = up_grad.astype(BF)
    rest = jnp.concatenate([hidden_grad[:, A:], hidden_grad[:, A:]], axis=1)
    gate_grad, up_grad = pair_grads(rest, gate_2, up_2)
    lane = lax.broadcasted_iota(jnp.int32, gate_grad.shape, 1)
    gu[g, :, 2 * A :] = jnp.where(lane < B, gate_grad, pltpu.roll(up_grad, B, 1)).astype(BF)

    grp_ag_start(7, gu, at_g, G_ORDER[1:])

    def s10_first(k):
        i = grp_arrived(7, gu, k)
        gi_f[...] = dot(gu[i], w_sp[...], 1, 0)
        for m in range(2):
            for j in range(XH):
                q = j * 2 + m
                gi_cs[m, i, j] = gi_f[q * RB : (q + 1) * RB, :].astype(BF)
        c_copy((3, i), gi_cs.at[o, i], gi_cr.at[i]).start()

    def s10_second(k):
        i = grp_from(k)
        c_copy((3, i), gi_cs.at[o, i], gi_cr.at[i]).wait_recv()
        for j in range(XH):
            gi_rs[i * XH + j] = (gi_cs[c, i, j].astype(FL) + gi_cr[i, j].astype(FL)).astype(BF)
            tp_send(7, i, j, gi_rs, gi_rr)

    lagged(G_ORDER, s10_first, s10_second)
    pair_sent(3, gi_cs, gi_cr)
    tp_sent(7, gi_rs, gi_rr)
    gut = gu[...].reshape(half, 2 * FS_L).T
    v_gg[:A] = dot(gut[:A], x[...], 1, 0)
    v_gg[A:] = dot(gut[2 * A : 2 * A + B], x[...], 1, 0)
    put(2, v_gg, o_gg)
    v_ug[:A] = dot(gut[A : 2 * A], x[...], 1, 0)
    v_ug[A:] = dot(gut[2 * A + B :], x[...], 1, 0)
    put(3, v_ug, o_ug)
    for wait in late:
        wait()
    late.clear()
    gi[...] = tp_rs_sum(7, gi_rs, gi_rr)
    put(4, gi, o_gi)
    for wait in late:
        wait()


def finish(*refs):
    n = len(refs) // 3
    sources, results, held, sem = refs[:n], refs[n : 2 * n], refs[2 * n : 3 * n], refs[-1]
    loads = [pltpu.make_async_copy(sources[i], held[i], sem.at[0, i]) for i in range(n)]
    stores = [pltpu.make_async_copy(held[i], results[i], sem.at[1, i]) for i in range(n)]
    for load in loads:
        load.start()
    for load, store in zip(loads, stores):
        load.wait()
        store.start()
    for store in stores:
        store.wait()


def body(
    sizes,
    teacher_in,
    teacher_gate,
    teacher_up,
    teacher_down,
    student_in,
    student_gate,
    student_up,
    student_down,
    projector,
):
    Y, XL, Z, XH = sizes
    G, N = Y * XL, Z * XH
    rb, kt = teacher_in.shape
    ft = teacher_gate.shape[1]
    bt = teacher_down.shape[1]
    ks = student_in.shape[1]
    fs = student_gate.shape[1]
    ds = student_down.shape[1]
    off = projector.shape[2]
    R = rb * N * 2
    rz, rg = R // Z, R // G
    q = ds // (2 * XH)
    proj_t = projector.transpose(1, 2, 0).reshape(-1, projector.shape[0])
    A = fs // 128 * 128
    V = pltpu.VMEM
    D = pltpu.SemaphoreType.DMA
    pair = lambda dt: [
        V((2, Z, rz, ds // 2), FL), V((2, Z, rz, ds // 2), dt), V((Z, rz, ds // 2), dt),
        V((N, rz, q), dt), V((N - 1, rz, q), dt), V((R, ds), dt),
    ]
    scratch = [
        V((kt, ft), BF), V((kt, ft), BF), V((ft, bt), BF), V((bt, ft), BF),
        V((2 * fs, ks), BF), V((fs, ds), BF), V((G * off, ds), BF),
        V((Z, XH, 2, rb, ks), BF), V((rz, ks), FL), V((R, ks), BF),
        V((G, rg, 2 * fs), BF), V((G - 1, rg, 2 * fs), BF), V((rg, 4 * fs - 2 * A), FL),
        V((G, rg, fs), BF),
        *pair(BF),
        V((G, off, R), BF), V((G - 1, off, R), BF), V((G, off, R), BF),
        *pair(BF),
        V((G, rg, fs), BF), V((G - 1, rg, fs), BF), V((G, rg, 2 * fs), BF), V((R, G * off), BF), V((G * off, ds), FL), V((fs, ds), FL), V((fs, ks), FL), V((fs, ks), FL),
        V((rz, ks), FL), V((2, Z, XH, rb, ks), BF), V((Z, XH, rb, ks), BF), V((N, rb, ks), BF),
        V((N - 1, rb, ks), BF), V((rb, ks), FL),
        V((Z, XH, 2, rb, kt), BF), V((rz, kt), FL), V((R, kt), BF),
        V((G, 2, rg, ft), BF), V((G - 1, 2, rg, ft), BF), V((2, rg, ft), FL), V((G, rg, ft), BF),
        V((2, Z, XH, off, R), FL), V((2, Z, XH, off, R), BF), V((Z, XH, off, R), BF), V((N, off, R), BF),
        V((N - 1, off, R), BF), V((off, R), FL),
        D((9,)), D((2,)), D((8,)), D((8, G)), D((8, G)), D((8, N)), D((8, N)),
        D((8, N)), D((8, N)), D((4, Z)), D((4, Z)),
    ]
    S = jax.ShapeDtypeStruct
    grads = pl.pallas_call(
        functools.partial(kernel, sizes),
        out_shape=(
            S((G * off, ds), FL), S((fs, ds), FL), S((fs, ks), FL), S((fs, ks), FL), S((rb, ks), FL),
        ),
        in_specs=[pl.BlockSpec(memory_space=pl.ANY)] * 9,
        out_specs=tuple([pl.BlockSpec(memory_space=pl.ANY)] * 5),
        scratch_shapes=scratch,
        compiler_params=pltpu.CompilerParams(
            collective_id=0, has_side_effects=True, vmem_limit_bytes=60 * 1024 * 1024
        ),
        name="chain",
    )(
        teacher_in, teacher_gate, teacher_up, teacher_down,
        student_in, student_gate.T, student_up.T, student_down, proj_t,
    )
    shapes = [(g.shape, g.dtype) for g in grads]
    grad_projector, grad_down, grad_gate, grad_up, grad_input = pl.pallas_call(
        finish,
        out_shape=tuple(S(*shape) for shape in shapes),
        in_specs=[pl.BlockSpec(memory_space=pl.ANY)] * 5,
        out_specs=tuple([pl.BlockSpec(memory_space=pl.ANY)] * 5),
        scratch_shapes=[*(V(*shape) for shape in shapes), D((2, 5))],
        compiler_params=pltpu.CompilerParams(vmem_limit_bytes=60 * 1024 * 1024),
        name="finish",
    )(*grads)
    grad_projector = grad_projector.reshape(G, off, ds).transpose(2, 0, 1)
    return grad_input, grad_gate.T, grad_up.T, grad_down, grad_projector


def solution(mesh, sizes=(4, 2, 8, 2)):
    torus = Mesh(mesh.devices.reshape(*sizes, 2), AXES)
    in_specs = (
        P(TP, GRP),
        P(GRP, TP),
        P(GRP, TP),
        P(TP, GRP),
        P(TP, GRP),
        P(GRP, TP),
        P(GRP, TP),
        P(TP, GRP),
        P(GRP, None, TP),
    )
    out_specs = (P(TP, GRP), P(GRP, TP), P(GRP, TP), P(TP, GRP), P(GRP, None, TP))
    return jax.shard_map(
        functools.partial(body, sizes), mesh=torus, in_specs=in_specs, out_specs=out_specs, check_vma=False
    )
```
